32 devices in a mesh: tp: 4 (over z), dp: 8 (over y, x, core).
Axes of the slice: x: 2, y: 2, z: 4, core: 2. Of those that a mesh axis runs over, the one named last changes fastest.
Arguments:
- hidden: bfloat16 [32, 128, 8192], P('dp')
- positions: int32 [128], replicated
- ln1_gain: bfloat16 [8192], replicated
- ln1_bias: bfloat16 [8192], replicated
- w_q: bfloat16 [8192, 8192], P(None, 'tp')
- w_k: bfloat16 [8192, 1024], P(None, 'tp')
- w_v: bfloat16 [8192, 1024], P(None, 'tp')
- w_o: bfloat16 [8192, 8192], P('tp')
- ln2_gain: bfloat16 [8192], replicated
- ln2_bias: bfloat16 [8192], replicated
- w_up: bfloat16 [8192, 32768], P(None, 'tp')
- w_down: bfloat16 [32768, 8192], P('tp')
Outputs:
- output 1: bfloat16 [32, 128, 8192], P('dp')
- output 2: float32 [32768], P('tp')
- output 3: float32 [64], P('tp')
- output 4: float32 [8192], replicated
All inputs are finite; a program needn't handle non-finite values.
Results may differ from the reference program's by a relative error of at most 0.0101556.
Values sent between devices are 32-bit elements.
A program may use at most 1.5 GiB of HBM per device.

```python
import jax
import jax.numpy as jnp
from jax import lax

D = 8192
HEADS = 64
KV_HEADS = 8
HEAD = 128
FF = 32768
SAMPLES = 32
SEQ_LEN = 128
POS_GAP = 64
ROT_DIM = HEAD // 2
ROPE_BASE = 10000.0
LN_EPS = 1e-5


def setup_inputs(seed: int = 0) -> dict:
    key_list = jax.random.split(jax.random.key(seed), 13)
    sample_shift = jax.random.normal(key_list[0], (SAMPLES, 1, D), jnp.float32)
    token_noise = jax.random.normal(key_list[1], (SAMPLES, SEQ_LEN, D), jnp.float32)
    hidden = (0.8 * sample_shift + 0.6 * token_noise).astype(jnp.bfloat16)
    pos_gaps = jax.random.randint(key_list[2], (SEQ_LEN,), 1, POS_GAP + 1)
    positions = (jnp.cumsum(pos_gaps) - pos_gaps[0]).astype(jnp.int32)

    def normal_weight(key_w, rows_in, cols_out):
        return (jax.random.normal(key_w, (rows_in, cols_out), jnp.float32) * rows_in ** -0.5).astype(jnp.bfloat16)

    def norm_param(key_w):
        return (0.3 * jax.random.normal(key_w, (D,), jnp.float32)).astype(jnp.bfloat16)

    return {
        "hidden": hidden,
        "positions": positions,
        "ln1_gain": norm_param(key_list[3]),
        "ln1_bias": norm_param(key_list[4]),
        "w_q": normal_weight(key_list[5], D, HEADS * HEAD),
        "w_k": normal_weight(key_list[6], D, KV_HEADS * HEAD),
        "w_v": normal_weight(key_list[7], D, KV_HEADS * HEAD),
        "w_o": normal_weight(key_list[8], HEADS * HEAD, D),
        "ln2_gain": norm_param(key_list[9]),
        "ln2_bias": norm_param(key_list[10]),
        "w_up": normal_weight(key_list[11], D, FF),
        "w_down": normal_weight(key_list[12], FF, D),
    }


def layer_norm_1p(in_rows, ln_gain, ln_bias):
    rows_f32 = in_rows.astype(jnp.float32)
    row_mean = jnp.mean(rows_f32, axis=-1, keepdims=True)
    centered = rows_f32 - row_mean
    row_var = jnp.mean(centered * centered, axis=-1, keepdims=True)
    scaled = centered * lax.rsqrt(row_var + LN_EPS)
    return (scaled * (1.0 + ln_gain.astype(jnp.float32)) + ln_bias.astype(jnp.float32)).astype(jnp.bfloat16)


def rope_tables(positions):
    rot_half = ROT_DIM // 2
    inv_freq = ROPE_BASE ** (-2.0 * jnp.arange(rot_half, dtype=jnp.float32) / ROT_DIM)
    pos_angle = positions.astype(jnp.float32)[:, None] * inv_freq[None, :]
    return jnp.cos(pos_angle), jnp.sin(pos_angle)


def apply_rope(heads_in, cos_b, sin_b):
    rot_half = ROT_DIM // 2
    heads_f32 = heads_in.astype(jnp.float32)
    lead_half = heads_f32[..., :rot_half]
    tail_half = heads_f32[..., rot_half:ROT_DIM]
    turned = jnp.concatenate([lead_half * cos_b - tail_half * sin_b, tail_half * cos_b + lead_half * sin_b], axis=-1)
    return jnp.concatenate([turned.astype(jnp.bfloat16), heads_in[..., ROT_DIM:]], axis=-1)


def reference(hidden, positions, ln1_gain, ln1_bias, w_q, w_k, w_v, w_o, ln2_gain, ln2_bias, w_up, w_down):
    q_group = HEADS // KV_HEADS
    cos_t, sin_t = rope_tables(positions)
    cos_b = cos_t[:, None, :]
    sin_b = sin_t[:, None, :]
    causal = jnp.arange(SEQ_LEN)[:, None] >= jnp.arange(SEQ_LEN)[None, :]

    def one_sample(x_rows):
        h_in = layer_norm_1p(x_rows, ln1_gain, ln1_bias)
        q_proj = jnp.dot(h_in, w_q, preferred_element_type=jnp.float32).astype(jnp.bfloat16).reshape(SEQ_LEN, HEADS, HEAD)
        k_proj = jnp.dot(h_in, w_k, preferred_element_type=jnp.float32).astype(jnp.bfloat16).reshape(SEQ_LEN, KV_HEADS, HEAD)
        v_proj = jnp.dot(h_in, w_v, preferred_element_type=jnp.float32).astype(jnp.bfloat16).reshape(SEQ_LEN, KV_HEADS, HEAD)
        q_proj = apply_rope(q_proj, cos_b, sin_b)
        k_proj = apply_rope(k_proj, cos_b, sin_b)
        k_full = jnp.repeat(k_proj, q_group, axis=1)
        v_full = jnp.repeat(v_proj, q_group, axis=1)
        scores = jnp.einsum("qhd,khd->hqk", q_proj.astype(jnp.float32), k_full.astype(jnp.float32)) * HEAD ** -0.5
        scores = jnp.where(causal[None, :, :], scores, -1e30)
        attn_prob = jax.nn.softmax(scores, axis=-1).astype(jnp.bfloat16)
        attn_out = jnp.einsum("hqk,khd->qhd", attn_prob.astype(jnp.float32), v_full.astype(jnp.float32)).astype(jnp.bfloat16)
        head_norm = jnp.sqrt(jnp.sum(jnp.square(attn_out.astype(jnp.float32)), axis=-1))
        o_sum = jnp.dot(attn_out.reshape(SEQ_LEN, HEADS * HEAD), w_o, preferred_element_type=jnp.float32)
        x_mid = (x_rows.astype(jnp.float32) + o_sum).astype(jnp.bfloat16)
        h_mid = layer_norm_1p(x_mid, ln2_gain, ln2_bias)
        mlp_act = jnp.square(jax.nn.relu(jnp.dot(h_mid, w_up, preferred_element_type=jnp.float32)))
        mlp_sum = jnp.dot(mlp_act.astype(jnp.bfloat16), w_down, preferred_element_type=jnp.float32)
        out_rows = (x_mid.astype(jnp.float32) + mlp_sum).astype(jnp.bfloat16)
        sample_means = (
            jnp.mean(mlp_act, axis=0),
            jnp.mean(head_norm, axis=0),
            jnp.mean(h_in.astype(jnp.float32), axis=0),
            jnp.mean(h_mid.astype(jnp.float32), axis=0),
        )
        return out_rows, sample_means

    out_hidden, mean_tuple = lax.map(one_sample, hidden)
    act_mean, head_mean, ln1_mean, ln2_mean = mean_tuple
    f_neuron = jnp.sqrt(jnp.sum(jnp.square(act_mean), axis=0))
    f_head = jnp.sqrt(jnp.sum(jnp.square(head_mean), axis=0))
    f_embed = jnp.sqrt(jnp.sum(jnp.square(ln1_mean), axis=0) + jnp.sum(jnp.square(ln2_mean), axis=0))
    return out_hidden, f_neuron, f_head, f_embed
```

```python
import functools

import jax
import jax.numpy as jnp
from jax import lax
from jax.experimental import pallas as pl
from jax.experimental.pallas import tpu as pltpu
from jax.sharding import PartitionSpec as P

HEAD_DIM = 128
ROT_DIM = 64
ROPE_BASE = 10000.0
LN_EPS = 1e-5
MESH = pl.DeviceIdType.MESH

ITEM_COLS = 256
SKEW = 2
SLOTS = 8
LN_PARTS = 4


def layer_norm_1p(in_rows, ln_gain, ln_bias):
    rows_f32 = in_rows.astype(jnp.float32)
    row_mean = jnp.mean(rows_f32, axis=-1, keepdims=True)
    centered = rows_f32 - row_mean
    row_var = jnp.mean(centered * centered, axis=-1, keepdims=True)
    scaled = centered * lax.rsqrt(row_var + LN_EPS)
    return (scaled * (1.0 + ln_gain.astype(jnp.float32)) + ln_bias.astype(jnp.float32)).astype(jnp.bfloat16)


def rope_tables(positions):
    rot_half = ROT_DIM // 2
    inv_freq = ROPE_BASE ** (-2.0 * jnp.arange(rot_half, dtype=jnp.float32) / ROT_DIM)
    pos_angle = positions.astype(jnp.float32)[:, None] * inv_freq[None, :]
    return jnp.cos(pos_angle), jnp.sin(pos_angle)


def apply_rope(heads_in, cos_b, sin_b):
    rot_half = ROT_DIM // 2
    heads_f32 = heads_in.astype(jnp.float32)
    lead_half = heads_f32[..., :rot_half]
    tail_half = heads_f32[..., rot_half:ROT_DIM]
    turned = jnp.concatenate([lead_half * cos_b - tail_half * sin_b, tail_half * cos_b + lead_half * sin_b], axis=-1)
    return jnp.concatenate([turned.astype(jnp.bfloat16), heads_in[..., ROT_DIM:]], axis=-1)


def attention_block(h_in, positions, w_q, w_k, w_v):
    n_batch = h_in.shape[0]
    n_seq = h_in.shape[1]
    kv_heads = w_k.shape[1] // HEAD_DIM
    q_group = w_q.shape[1] // w_k.shape[1]
    cos_t, sin_t = rope_tables(positions)
    q_proj = jnp.einsum("bsd,dn->bsn", h_in, w_q, preferred_element_type=jnp.float32).astype(jnp.bfloat16)
    q_proj = q_proj.reshape(n_batch, n_seq, kv_heads, q_group, HEAD_DIM)
    k_proj = jnp.einsum("bsd,dn->bsn", h_in, w_k, preferred_element_type=jnp.float32).astype(jnp.bfloat16)
    k_proj = k_proj.reshape(n_batch, n_seq, kv_heads, HEAD_DIM)
    v_proj = jnp.einsum("bsd,dn->bsn", h_in, w_v, preferred_element_type=jnp.float32).astype(jnp.bfloat16)
    v_proj = v_proj.reshape(n_batch, n_seq, kv_heads, HEAD_DIM)
    q_proj = apply_rope(q_proj, cos_t[None, :, None, None, :], sin_t[None, :, None, None, :])
    k_proj = apply_rope(k_proj, cos_t[None, :, None, :], sin_t[None, :, None, :])
    scores = jnp.einsum("bqkgd,bskd->bkgqs", q_proj, k_proj, preferred_element_type=jnp.float32) * HEAD_DIM ** -0.5
    causal = jnp.arange(n_seq)[:, None] >= jnp.arange(n_seq)[None, :]
    scores = jnp.where(causal, scores, -1e30)
    attn_prob = jax.nn.softmax(scores, axis=-1).astype(jnp.bfloat16)
    return jnp.einsum("bkgqs,bskd->bqkgd", attn_prob, v_proj, preferred_element_type=jnp.float32).astype(jnp.bfloat16)


def tail_kernel(
    dims,
    attn_hbm, x_hbm, wo_hbm, wup_hbm, wdn_hbm, gain_ref, bias_ref, pay_in,
    y_hbm, score_ref,
    attn, xbuf, part, lhs, wbuf, rslot, bslot, acc8, pay, recvpay,
    in_sem, w_sem, r_send, r_recv, b_send, b_recv, p_send, p_recv, r_cred, b_cred,
):
    tp, dp, n_seq, width, k_attn, n_items, n_chunks = dims
    z = lax.axis_index("tp")
    d = lax.axis_index("dp")
    last = tp - 1
    cw = width // n_items
    bw = 2 * cw
    n_blk = width // bw
    rows = 2 * n_seq
    total = 2 * n_chunks * n_items
    lag = 2 * last * SKEW

    barrier = pltpu.get_barrier_semaphore()
    for o in range(1, tp):
        pl.semaphore_signal(barrier, inc=1, device_id={"tp": lax.rem(z + o, tp)}, device_id_type=MESH)
    for o in range(1, dp):
        pl.semaphore_signal(barrier, inc=1, device_id={"dp": lax.rem(d + o, dp)}, device_id_type=MESH)

    attn_copy = pltpu.make_async_copy(attn_hbm, attn, in_sem.at[0])
    x_copy = pltpu.make_async_copy(x_hbm, xbuf, in_sem.at[1])

    def wo_copy(b, slot):
        cols = pl.ds(pl.multiple_of(b * bw, bw), bw)
        return pltpu.make_async_copy(wo_hbm.at[:, cols], wbuf.at[slot, pl.ds(0, k_attn), :], w_sem.at[slot])

    def w_copy(hbm, b, slot):
        cols = pl.ds(pl.multiple_of(b * bw, bw), bw)
        return pltpu.make_async_copy(hbm.at[:, cols], wbuf.at[slot], w_sem.at[slot])

    def start_w(k):
        slot = lax.rem(k, 2)
        kk = lax.rem(k, 2 * n_blk)

        @pl.when(kk < n_blk)
        def _():
            w_copy(wup_hbm, kk, slot).start()

        @pl.when(kk >= n_blk)
        def _():
            w_copy(wdn_hbm, kk - n_blk, slot).start()

    def out_proj(b):
        slot = lax.rem(b, 2)
        wo_copy(b, slot).wait()
        acc = jnp.dot(attn[...], wbuf[slot, 0:k_attn, :], preferred_element_type=jnp.float32)
        for c in range(n_chunks):
            for g in range(2):
                for half in range(2):
                    r0 = (2 * c + g) * n_seq
                    part[(2 * c + g) * n_items + 2 * b + half] = acc[r0:r0 + n_seq, half * cw:(half + 1) * cw]

        @pl.when(b + 2 < n_blk)
        def _():
            wo_copy(b + 2, slot).start()

        @pl.when(b + 2 >= n_blk)
        def _():
            start_w(b + 2 - n_blk)

    attn_copy.start()
    wo_copy(0, 0).start()
    wo_copy(1, 1).start()
    x_copy.start()
    pay[...] = pay_in[...]
    attn_copy.wait()
    out_proj(0)
    x_copy.wait()
    pl.semaphore_wait(barrier, tp - 1 + dp - 1)

    def tile_of(t, g):
        c = lax.rem(lax.div(t, n_items), n_chunks)
        i = lax.rem(t, n_items)
        row = pl.multiple_of((2 * c + g) * n_seq, n_seq)
        col = pl.multiple_of(i * cw, cw)
        return (2 * c + g) * n_items + i, pl.ds(row, n_seq), pl.ds(col, cw)

    def place(g):
        return z if g == 0 else last - z

    def onward(g):
        return {"tp": z + 1} if g == 0 else {"tp": z - 1}

    def backward(g):
        return {"tp": z - 1} if g == 0 else {"tp": z + 1}

    def r_copy(g, t, src):
        slot = lax.rem(t, SLOTS)
        return pltpu.make_async_remote_copy(
            src_ref=src, dst_ref=rslot.at[g, slot], send_sem=r_send.at[g, slot], recv_sem=r_recv.at[g, slot],
            device_id=onward(g), device_id_type=MESH,
        )

    def b_copy(g, t, src):
        slot = lax.rem(t, SLOTS)
        return pltpu.make_async_remote_copy(
            src_ref=src, dst_ref=bslot.at[g, slot], send_sem=b_send.at[g, slot], recv_sem=b_recv.at[g, slot],
            device_id=backward(g), device_id_type=MESH,
        )

    def r_arrive(g, t, p):
        slot = lax.rem(t, SLOTS)
        idx, rws, cls = tile_of(t, g)

        @pl.when((p == 1) | (p == 2))
        def _():
            r_copy(g, t, rslot.at[g, slot]).wait_recv()
            rslot[g, slot] = rslot[g, slot] + part[idx]

        @pl.when(p == last)
        def _():
            r_copy(g, t, rslot.at[g, slot]).wait_recv()
            new = (xbuf[rws, cls].astype(jnp.float32) + (rslot[g, slot] + part[idx])).astype(jnp.bfloat16)
            xbuf[rws, cls] = new
            rslot[g, slot] = new.astype(jnp.float32)

    def r_leave(g, t, p):
        slot = lax.rem(t, SLOTS)
        old = t - SKEW
        old_slot = lax.rem(old + SLOTS, SLOTS)
        idx, _, _ = tile_of(t, g)

        @pl.when((p == 0) & (t >= SLOTS))
        def _():
            r_copy(g, t, part.at[idx]).wait_send()

        @pl.when((p < last) & (t >= SLOTS))
        def _():
            pl.semaphore_wait(r_cred.at[g], 1)

        @pl.when(p == 0)
        def _():
            r_copy(g, t, part.at[idx]).start()

        @pl.when((p == 1) | (p == 2))
        def _():
            r_copy(g, t, rslot.at[g, slot]).start()

        @pl.when((p == last) & (t >= SLOTS))
        def _():
            pl.semaphore_wait(b_cred.at[g], 1)

        @pl.when(p == last)
        def _():
            b_copy(g, t, rslot.at[g, slot]).start()

        @pl.when(((p == 1) | (p == 2)) & (old >= 0))
        def _():
            r_copy(g, old, rslot.at[g, old_slot]).wait_send()

        @pl.when((p == last) & (old >= 0))
        def _():
            b_copy(g, old, rslot.at[g, old_slot]).wait_send()

        @pl.when((p > 0) & (old >= 0) & (old < total - SLOTS))
        def _():
            pl.semaphore_signal(r_cred.at[g], inc=1, device_id=backward(g), device_id_type=MESH)

    def b_step(g, t, p):
        slot = lax.rem(t, SLOTS)
        old = t - SKEW
        old_slot = lax.rem(old + SLOTS, SLOTS)
        _, rws, cls = tile_of(t, g)
        b_copy(g, t, bslot.at[g, slot]).wait_recv()

        @pl.when((p > 0) & (t >= SLOTS))
        def _():
            pl.semaphore_wait(b_cred.at[g], 1)

        @pl.when(p > 0)
        def _():
            b_copy(g, t, bslot.at[g, slot]).start()

        xbuf[rws, cls] = bslot[g, slot].astype(jnp.bfloat16)

        @pl.when((p > 0) & (old >= 0))
        def _():
            b_copy(g, old, bslot.at[g, old_slot]).wait_send()

        @pl.when((old >= 0) & (old < total - SLOTS))
        def _():
            pl.semaphore_signal(b_cred.at[g], inc=1, device_id=onward(g), device_id_type=MESH)

    def service(s):
        for g in range(2):
            p = place(g)
            t = s - SKEW * p

            @pl.when((t >= 0) & (t < total))
            def _(g=g, p=p, t=t):
                r_arrive(g, t, p)

        for g in range(2):
            p = place(g)
            t = s - SKEW * (2 * last - p)

            @pl.when((p < last) & (t >= 0) & (t < total))
            def _(g=g, p=p, t=t):
                b_step(g, t, p)

        for g in range(2):
            p = place(g)
            t = s - SKEW * p

            @pl.when((t >= 0) & (t < total))
            def _(g=g, p=p, t=t):
                r_leave(g, t, p)

    lane = 512 if width % 512 == 0 else 128
    n_lane = width // lane
    ln_rows = rows // LN_PARTS
    seq_parts = n_seq // ln_rows

    def ln_part(c, q):
        @pl.when(lax.rem(q, seq_parts) == 0)
        def _():
            acc8[...] = jnp.zeros_like(acc8)

        def group(r, carry):
            src = pl.ds(pl.multiple_of(c * rows + q * ln_rows + r * 16, 16), 16)
            dst = pl.ds(pl.multiple_of(q * ln_rows + r * 16, 16), 16)
            tot = jnp.zeros((16, lane), jnp.float32)
            for j in range(n_lane):
                tot = tot + xbuf[src, j * lane:(j + 1) * lane].astype(jnp.float32)
            mean = jnp.sum(tot, axis=-1, keepdims=True) * (1.0 / width)
            var = jnp.zeros((16, lane), jnp.float32)
            for j in range(n_lane):
                cen = xbuf[src, j * lane:(j + 1) * lane].astype(jnp.float32) - mean
                var = var + cen * cen
            rstd = lax.rsqrt(jnp.sum(var, axis=-1, keepdims=True) * (1.0 / width) + LN_EPS)
            for j in range(n_lane):
                cl = slice(j * lane, (j + 1) * lane)
                cen = xbuf[src, cl].astype(jnp.float32) - mean
                h = ((cen * rstd) * (1.0 + gain_ref[:, cl]) + bias_ref[:, cl]).astype(jnp.bfloat16)
                lhs[0, dst, cl] = h
                hf = h.astype(jnp.float32)
                acc8[:, cl] = acc8[:, cl] + (hf[0:8] + hf[8:16])
            return carry

        lax.fori_loop(0, ln_rows // 16, group, 0)

        @pl.when(lax.rem(q, seq_parts) == seq_parts - 1)
        def _():
            m = jnp.sum(acc8[...], axis=0, keepdims=True) * (1.0 / n_seq)
            pay[:, width:2 * width] = pay[:, width:2 * width] + m * m

    def mlp_block(k):
        slot = lax.rem(k, 2)
        kk = lax.rem(k, 2 * n_blk)
        c = lax.div(k, 2 * n_blk)
        second = lax.div(kk, n_blk)
        b = kk - second * n_blk
        w_copy(wup_hbm, b, slot).wait()
        acc = jnp.dot(lhs[second], wbuf[slot], preferred_element_type=jnp.float32)

        @pl.when(second == 0)
        def _():
            relu = jnp.maximum(acc, 0.0)
            act = relu * relu
            cols = pl.ds(pl.multiple_of(b * bw, bw), bw)
            m0 = jnp.sum(act[0:n_seq], axis=0, keepdims=True) * (1.0 / n_seq)
            m1 = jnp.sum(act[n_seq:rows], axis=0, keepdims=True) * (1.0 / n_seq)
            pay[:, cols] = pay[:, cols] + (m0 * m0 + m1 * m1)
            lhs[1, :, cols] = act.astype(jnp.bfloat16)

        @pl.when(second == 1)
        def _():
            for g in range(2):
                for half in range(2):
                    part[(2 * c + g) * n_items + 2 * b + half] = acc[
                        g * n_seq:(g + 1) * n_seq, half * cw:(half + 1) * cw
                    ]

        @pl.when(k + 2 < 2 * n_blk * n_chunks)
        def _():
            start_w(k + 2)

    def pay_copy(peer, src_d, o):
        return pltpu.make_async_remote_copy(
            src_ref=pay, dst_ref=recvpay.at[src_d], send_sem=p_send.at[o], recv_sem=p_recv.at[src_d],
            device_id={"dp": peer}, device_id_type=MESH,
        )

    def y_copy(c):
        r = pl.ds(c * rows, rows)
        return pltpu.make_async_copy(xbuf.at[r, :], y_hbm.at[r, :], in_sem.at[c])

    ln_at = n_items - 1 + lag
    mlp_at = ln_at + LN_PARTS
    n_mlp = 2 * n_blk * n_chunks
    pay_at = mlp_at + n_mlp - n_blk + 2

    def step(s, carry):
        service(s)

        @pl.when(s + 1 < n_blk)
        def _():
            out_proj(s + 1)

        for c in range(n_chunks):
            q = s - ln_at - c * n_items

            @pl.when((q >= 0) & (q < LN_PARTS))
            def _(c=c, q=q):
                ln_part(c, q)

        k = s - mlp_at

        @pl.when((k >= 0) & (k < n_mlp))
        def _():
            mlp_block(k)

        @pl.when(s == pay_at)
        def _():
            for o in range(1, dp):
                pay_copy(lax.rem(d + o, dp), d, o).start()
            recvpay[d] = pay[...]

        for c in range(n_chunks - 1):
            @pl.when(s == total - 1 + lag - (n_chunks - 1 - c) * n_items)
            def _(c=c):
                y_copy(c).start()

        return carry

    lax.fori_loop(0, total + lag, step, 0)

    y_copy(n_chunks - 1).start()
    for o in range(1, dp):
        src_d = lax.rem(d + o, dp)
        pay_copy(src_d, src_d, o).wait_recv()
    score = recvpay[0]
    for j in range(1, dp):
        score = score + recvpay[j]
    score_ref[...] = score
    for o in range(1, dp):
        pay_copy(lax.rem(d + o, dp), d, o).wait_send()
    for g in range(2):
        p = place(g)
        for back in range(SLOTS):
            t = total - 1 - back
            slot = t % SLOTS

            @pl.when(p == 0)
            def _(g=g, t=t, slot=slot):
                r_copy(g, t, part.at[0]).wait_send()

            if back < SKEW:
                @pl.when((p == 1) | (p == 2))
                def _(g=g, t=t, slot=slot):
                    r_copy(g, t, rslot.at[g, slot]).wait_send()
                    b_copy(g, t, bslot.at[g, slot]).wait_send()

                @pl.when(p == last)
                def _(g=g, t=t, slot=slot):
                    b_copy(g, t, rslot.at[g, slot]).wait_send()
    for c in range(n_chunks):
        y_copy(c).wait()


def layer_tail(tp, dp, attn, x_rows, w_o, w_up, w_down, gain, bias, pay, n_seq):
    tokens, width = x_rows.shape
    k_attn = attn.shape[1]
    n_items = width // ITEM_COLS
    n_chunks = tokens // (2 * n_seq)
    dims = (tp, dp, n_seq, width, k_attn, n_items, n_chunks)
    cw = ITEM_COLS
    hbm = pl.BlockSpec(memory_space=pl.ANY)
    vmem = pl.BlockSpec(memory_space=pltpu.VMEM)
    dma = pltpu.SemaphoreType.DMA
    return pl.pallas_call(
        functools.partial(tail_kernel, dims),
        name="layer_tail",
        out_shape=(
            jax.ShapeDtypeStruct((tokens, width), jnp.bfloat16),
            jax.ShapeDtypeStruct(pay.shape, jnp.float32),
        ),
        in_specs=[hbm, hbm, hbm, hbm, hbm, vmem, vmem, vmem],
        out_specs=(hbm, vmem),
        scratch_shapes=[
            pltpu.VMEM((tokens, k_attn), jnp.bfloat16),
            pltpu.VMEM((tokens, width), jnp.bfloat16),
            pltpu.VMEM((2 * n_chunks * n_items, n_seq, cw), jnp.float32),
            pltpu.VMEM((2, 2 * n_seq, width), jnp.bfloat16),
            pltpu.VMEM((2, width, 2 * cw), jnp.bfloat16),
            pltpu.VMEM((2, SLOTS, n_seq, cw), jnp.float32),
            pltpu.VMEM((2, SLOTS, n_seq, cw), jnp.float32),
            pltpu.VMEM((8, width), jnp.float32),
            pltpu.VMEM(pay.shape, jnp.float32),
            pltpu.VMEM((dp,) + pay.shape, jnp.float32),
            dma((2,)), dma((2,)),
            dma((2, SLOTS)), dma((2, SLOTS)), dma((2, SLOTS)), dma((2, SLOTS)),
            dma((dp,)), dma((dp,)),
            pltpu.SemaphoreType.REGULAR((2,)), pltpu.SemaphoreType.REGULAR((2,)),
        ],
        compiler_params=pltpu.CompilerParams(
            collective_id=0, has_side_effects=True, vmem_limit_bytes=66_000_000
        ),
        cost_estimate=pl.CostEstimate(
            flops=2 * tokens * width * (k_attn + 2 * width),
            bytes_accessed=2 * width * (k_attn + 4 * width),
            transcendentals=0,
        ),
    )(attn, x_rows, w_o, w_up, w_down, gain, bias, pay)


def solution(mesh):
    tp = mesh.shape["tp"]
    dp = mesh.shape["dp"]

    def local_layer(hidden, positions, ln1_gain, ln1_bias, w_q, w_k, w_v, w_o, ln2_gain, ln2_bias, w_up, w_down):
        n_batch, n_seq, width = hidden.shape
        ff_local = w_up.shape[1]
        h_in = layer_norm_1p(hidden, ln1_gain, ln1_bias)
        attn_out = attention_block(h_in, positions, w_q, w_k, w_v)
        head_norm = jnp.sqrt(jnp.sum(jnp.square(attn_out.astype(jnp.float32)), axis=-1)).reshape(n_batch, n_seq, -1)
        head_sq = jnp.sum(jnp.square(jnp.mean(head_norm, axis=1)), axis=0)
        ln1_sq = jnp.sum(jnp.square(jnp.mean(h_in, axis=1, dtype=jnp.float32)), axis=0)
        heads = head_sq.shape[0]
        pay = jnp.concatenate(
            [jnp.zeros((ff_local,), jnp.float32), ln1_sq, head_sq, jnp.zeros((128 - heads,), jnp.float32)]
        ).reshape(1, -1)
        y_rows, score = layer_tail(
            tp, dp,
            attn_out.reshape(n_batch * n_seq, -1),
            hidden.reshape(n_batch * n_seq, width),
            w_o, w_up, w_down,
            ln2_gain.astype(jnp.float32).reshape(1, width),
            ln2_bias.astype(jnp.float32).reshape(1, width),
            pay, n_seq,
        )
        roots = jnp.sqrt(score.reshape(-1))
        return (
            y_rows.reshape(n_batch, n_seq, width),
            roots[:ff_local],
            roots[ff_local + width:ff_local + width + heads],
            roots[ff_local:ff_local + width],
        )

    weight_col = P(None, "tp")
    weight_row = P("tp", None)
    return jax.shard_map(
        local_layer,
        mesh=mesh,
        in_specs=(P("dp"), P(), P(), P(), weight_col, weight_col, weight_col, weight_row, P(), P(), weight_col, weight_row),
        out_specs=(P("dp"), P("tp"), P("tp"), P()),
        check_vma=False,
    )
```

```python
import functools

import jax
import jax.numpy as jnp
from jax import lax
from jax.experimental import pallas as pl
from jax.experimental.pallas import tpu as pltpu
from jax.sharding import PartitionSpec as P

HEAD_DIM = 128
ROT_DIM = 64
ROPE_BASE = 10000.0
LN_EPS = 1e-5
MESH = pl.DeviceIdType.MESH

ITEM_COLS = 256
SKEW = 2
SLOTS = 8
LN_PARTS = 4
VMEM_BYTES = 52 << 20
LN1_AT = 8


def rope_tables(positions):
    rot_half = ROT_DIM // 2
    lane_id = jnp.arange(HEAD_DIM)
    pair = (lane_id % rot_half).astype(jnp.float32)
    inv_freq = ROPE_BASE ** (-2.0 * pair / ROT_DIM)
    pos_angle = positions.astype(jnp.float32)[:, None] * inv_freq[None, :]
    sign = jnp.where(lane_id < rot_half, -1.0, 1.0)
    return jnp.cos(pos_angle), jnp.sin(pos_angle) * sign[None, :]


def layer_kernel(
    dims,
    x_hbm, wq_hbm, wk_hbm, wv_hbm, wo_hbm, wup_hbm, wdn_hbm, gain1_ref, bias1_ref, gain2_ref, bias2_ref, cos_ref, sin_ref,
    xbuf, score_ref,
    attn, kbuf, vbuf, gains, biases, part, lhs, wbuf, rslot, bslot, acc8, pay, recvpay,
    in_sem, w_sem, r_send, r_recv, b_send, b_recv, p_send, p_recv, r_cred, b_cred,
):
    tp, dp, n_seq, width, k_attn, kv_width, n_items = dims
    n_chunks = 2
    z = lax.axis_index("tp")
    d = lax.axis_index("dp")
    last = tp - 1
    cw = width // n_items
    bw = 2 * cw
    n_blk = width // bw
    rows = 2 * n_seq
    total = 2 * n_chunks * n_items
    lag = 2 * last * SKEW

    barrier = pltpu.get_barrier_semaphore()
    for o in range(1, tp):
        pl.semaphore_signal(barrier, inc=1, device_id={"tp": lax.rem(z + o, tp)}, device_id_type=MESH)
    for o in range(1, dp):
        pl.semaphore_signal(barrier, inc=1, device_id={"dp": lax.rem(d + o, dp)}, device_id_type=MESH)

    def x_copy(c):
        r = pl.ds(c * rows, rows)
        return pltpu.make_async_copy(x_hbm.at[r, :], xbuf.at[r, :], in_sem.at[c])

    heads_blk = bw // HEAD_DIM
    n_q = k_attn // bw
    n_pre = 1 + n_q
    att_len = n_pre + n_blk
    n_att = n_chunks * att_len
    q_group = k_attn // kv_width

    def w_copy(hbm, b, slot):
        cols = pl.ds(pl.multiple_of(b * bw, bw), bw)
        return pltpu.make_async_copy(hbm.at[:, cols], wbuf.at[slot], w_sem.at[slot])

    def wo_copy(b, slot):
        cols = pl.ds(pl.multiple_of(b * bw, bw), bw)
        return pltpu.make_async_copy(wo_hbm.at[:, cols], wbuf.at[slot, pl.ds(0, k_attn), :], w_sem.at[slot])

    def k_copy(slot):
        return pltpu.make_async_copy(wk_hbm, wbuf.at[slot, :, pl.ds(0, kv_width)], w_sem.at[slot])

    def v_copy(slot):
        return pltpu.make_async_copy(wv_hbm, wbuf.at[slot, :, pl.ds(kv_width, kv_width)], w_sem.at[2])

    def start_block(idx):
        slot = lax.rem(idx, 2)

        @pl.when(idx < n_att)
        def _():
            j = lax.rem(idx, att_len)

            @pl.when(j == 0)
            def _():
                k_copy(slot).start()
                v_copy(slot).start()

            @pl.when((j > 0) & (j < n_pre))
            def _():
                w_copy(wq_hbm, j - 1, slot).start()

            @pl.when(j >= n_pre)
            def _():
                wo_copy(j - n_pre, slot).start()

        @pl.when((idx >= n_att) & (idx < n_att + n_mlp))
        def _():
            kk = lax.rem(idx - n_att, 2 * n_blk)

            @pl.when(kk < n_blk)
            def _():
                w_copy(wup_hbm, kk, slot).start()

            @pl.when(kk >= n_blk)
            def _():
                w_copy(wdn_hbm, kk - n_blk, slot).start()

    def rotate(heads):
        reps = heads.shape[0] // n_seq
        lane_id = lax.broadcasted_iota(jnp.int32, heads.shape, 1)
        quarter = ROT_DIM // 2
        partner = jnp.where(
            lane_id < quarter, pltpu.roll(heads, HEAD_DIM - quarter, 1), pltpu.roll(heads, quarter, 1)
        )
        cos_t = jnp.concatenate([cos_ref[...]] * reps, axis=0)
        sin_t = jnp.concatenate([sin_ref[...]] * reps, axis=0)
        return jnp.where(lane_id < ROT_DIM, heads * cos_t + partner * sin_t, heads).astype(jnp.bfloat16)

    def keys_values(slot):
        k_copy(slot).wait()
        v_copy(slot).wait()
        acc = jnp.dot(lhs[0], wbuf[slot], preferred_element_type=jnp.float32).astype(jnp.bfloat16)
        for g in range(2):
            r = slice(g * n_seq, (g + 1) * n_seq)
            for h in range(kv_width // HEAD_DIM):
                cl = slice(h * HEAD_DIM, (h + 1) * HEAD_DIM)
                kbuf[g, h] = rotate(acc[r, cl].astype(jnp.float32))
                vbuf[g, h] = acc[r, kv_width + h * HEAD_DIM:kv_width + (h + 1) * HEAD_DIM]

    def queries(jq, slot):
        w_copy(wq_hbm, jq, slot).wait()
        acc = jnp.dot(lhs[0], wbuf[slot], preferred_element_type=jnp.float32).astype(jnp.bfloat16)
        kv = lax.div(jq * heads_blk, q_group)
        shape = (heads_blk * n_seq, n_seq)
        causal = lax.rem(lax.broadcasted_iota(jnp.int32, shape, 0), n_seq) >= lax.broadcasted_iota(jnp.int32, shape, 1)
        lane_id = lax.broadcasted_iota(jnp.int32, (1, HEAD_DIM), 1)
        head_sq = jnp.zeros((1, HEAD_DIM), jnp.float32)
        for g in range(2):
            r = slice(g * n_seq, (g + 1) * n_seq)
            heads = jnp.concatenate(
                [acc[r, h * HEAD_DIM:(h + 1) * HEAD_DIM].astype(jnp.float32) for h in range(heads_blk)], axis=0
            )
            q_rot = rotate(heads)
            logits = lax.dot_general(
                q_rot, kbuf[g, kv], (((1,), (1,)), ((), ())), preferred_element_type=jnp.float32
            ) * HEAD_DIM ** -0.5
            logits = jnp.where(causal, logits, -1e30)
            weights = jnp.exp(logits - jnp.max(logits, axis=-1, keepdims=True))
            prob = (weights / jnp.sum(weights, axis=-1, keepdims=True)).astype(jnp.bfloat16)
            out = jnp.dot(prob, vbuf[g, kv], preferred_element_type=jnp.float32).astype(jnp.bfloat16)
            wide = out.astype(jnp.float32)
            norm = jnp.sqrt(jnp.sum(wide * wide, axis=-1, keepdims=True))
            for h in range(heads_blk):
                hr = slice(h * n_seq, (h + 1) * n_seq)
                attn[r, pl.ds(pl.multiple_of(jq * bw + h * HEAD_DIM, HEAD_DIM), HEAD_DIM)] = out[hr]
                m = jnp.sum(norm[hr], axis=0, keepdims=True) * (1.0 / n_seq)
                head_sq = head_sq + jnp.where(lane_id == jq * heads_blk + h, m * m, 0.0)
        pay[:, 2 * width:2 * width + HEAD_DIM] = pay[:, 2 * width:2 * width + HEAD_DIM] + head_sq

    def out_proj(c, b, slot):
        wo_copy(b, slot).wait()
        acc = jnp.dot(attn[...], wbuf[slot, 0:k_attn, :], preferred_element_type=jnp.float32)
        for g in range(2):
            for half in range(2):
                part[(2 * c + g) * n_items + 2 * b + half] = acc[
                    g * n_seq:(g + 1) * n_seq, half * cw:(half + 1) * cw
                ]

    def att_block(idx):
        slot = lax.rem(idx, 2)
        c = lax.div(idx, att_len)
        j = lax.rem(idx, att_len)

        @pl.when(j == 0)
        def _():
            keys_values(slot)

        @pl.when((j > 0) & (j < n_pre))
        def _():
            queries(j - 1, slot)

        @pl.when(j >= n_pre)
        def _():
            out_proj(c, j - n_pre, slot)

        start_block(idx + 2)

    n_mlp = 2 * n_blk * n_chunks
    x_copy(0).start()
    start_block(jnp.int32(0))
    start_block(jnp.int32(1))
    x_copy(1).start()
    pay[...] = jnp.zeros_like(pay)
    for which, (gain, bias) in enumerate(((gain1_ref, bias1_ref), (gain2_ref, bias2_ref))):
        gains[which] = 1.0 + gain[...].astype(jnp.float32)
        biases[which] = bias[...].astype(jnp.float32)
    x_copy(0).wait()
    pl.semaphore_wait(barrier, tp - 1 + dp - 1)

    def tile_of(t, g):
        c = lax.rem(lax.div(t, n_items), n_chunks)
        i = lax.rem(t, n_items)
        row = pl.multiple_of((2 * c + g) * n_seq, n_seq)
        col = pl.multiple_of(i * cw, cw)
        return (2 * c + g) * n_items + i, pl.ds(row, n_seq), pl.ds(col, cw)

    def place(g):
        return z if g == 0 else last - z

    def onward(g):
        return {"tp": z + 1} if g == 0 else {"tp": z - 1}

    def backward(g):
        return {"tp": z - 1} if g == 0 else {"tp": z + 1}

    def r_copy(g, t, src):
        slot = lax.rem(t, SLOTS)
        return pltpu.make_async_remote_copy(
            src_ref=src, dst_ref=rslot.at[g, slot], send_sem=r_send.at[g, slot], recv_sem=r_recv.at[g, slot],
            device_id=onward(g), device_id_type=MESH,
        )

    def b_copy(g, t, src):
        slot = lax.rem(t, SLOTS)
        return pltpu.make_async_remote_copy(
            src_ref=src, dst_ref=bslot.at[g, slot], send_sem=b_send.at[g, slot], recv_sem=b_recv.at[g, slot],
            device_id=backward(g), device_id_type=MESH,
        )

    def r_arrive(g, t, p):
        slot = lax.rem(t, SLOTS)
        idx, rws, cls = tile_of(t, g)

        @pl.when((p == 1) | (p == 2))
        def _():
            r_copy(g, t, rslot.at[g, slot]).wait_recv()
            rslot[g, slot] = rslot[g, slot] + part[idx]

        @pl.when(p == last)
        def _():
            r_copy(g, t, rslot.at[g, slot]).wait_recv()
            new = (xbuf[rws, cls].astype(jnp.float32) + (rslot[g, slot] + part[idx])).astype(jnp.bfloat16)
            xbuf[rws, cls] = new
            rslot[g, slot] = new.astype(jnp.float32)

    def r_leave(g, t, p):
        slot = lax.rem(t, SLOTS)
        old = t - SKEW
        old_slot = lax.rem(old + SLOTS, SLOTS)
        idx, _, _ = tile_of(t, g)

        @pl.when((p == 0) & (t >= SLOTS))
        def _():
            r_copy(g, t, part.at[idx]).wait_send()

        @pl.when((p < last) & (t >= SLOTS))
        def _():
            pl.semaphore_wait(r_cred.at[g], 1)

        @pl.when(p == 0)
        def _():
            r_copy(g, t, part.at[idx]).start()

        @pl.when((p == 1) | (p == 2))
        def _():
            r_copy(g, t, rslot.at[g, slot]).start()

        @pl.when((p == last) & (t >= SLOTS))
        def _():
            pl.semaphore_wait(b_cred.at[g], 1)

        @pl.when(p == last)
        def _():
            b_copy(g, t, rslot.at[g, slot]).start()

        @pl.when(((p == 1) | (p == 2)) & (old >= 0))
        def _():
            r_copy(g, old, rslot.at[g, old_slot]).wait_send()

        @pl.when((p == last) & (old >= 0))
        def _():
            b_copy(g, old, rslot.at[g, old_slot]).wait_send()

        @pl.when((p > 0) & (old >= 0) & (old < total - SLOTS))
        def _():
            pl.semaphore_signal(r_cred.at[g], inc=1, device_id=backward(g), device_id_type=MESH)

    def b_step(g, t, p):
        slot = lax.rem(t, SLOTS)
        old = t - SKEW
        old_slot = lax.rem(old + SLOTS, SLOTS)
        _, rws, cls = tile_of(t, g)
        b_copy(g, t, bslot.at[g, slot]).wait_recv()

        @pl.when((p > 0) & (t >= SLOTS))
        def _():
            pl.semaphore_wait(b_cred.at[g], 1)

        @pl.when(p > 0)
        def _():
            b_copy(g, t, bslot.at[g, slot]).start()

        xbuf[rws, cls] = bslot[g, slot].astype(jnp.bfloat16)

        @pl.when((p > 0) & (old >= 0))
        def _():
            b_copy(g, old, bslot.at[g, old_slot]).wait_send()

        @pl.when((old >= 0) & (old < total - SLOTS))
        def _():
            pl.semaphore_signal(b_cred.at[g], inc=1, device_id=onward(g), device_id_type=MESH)

    def service(s):
        for g in range(2):
            p = place(g)
            t = s - SKEW * p

            @pl.when((t >= 0) & (t < total))
            def _(g=g, p=p, t=t):
                r_arrive(g, t, p)

        for g in range(2):
            p = place(g)
            t = s - SKEW * (2 * last - p)

            @pl.when((p < last) & (t >= 0) & (t < total))
            def _(g=g, p=p, t=t):
                b_step(g, t, p)

        for g in range(2):
            p = place(g)
            t = s - SKEW * p

            @pl.when((t >= 0) & (t < total))
            def _(g=g, p=p, t=t):
                r_leave(g, t, p)

    lane = 512 if width % 512 == 0 else 128
    n_lane = width // lane
    ln_rows = rows // LN_PARTS
    seq_parts = n_seq // ln_rows

    def ln_part(which, c, q):
        @pl.when(lax.rem(q, seq_parts) == 0)
        def _():
            acc8[...] = jnp.zeros_like(acc8)

        def group(r, carry):
            src = pl.ds(pl.multiple_of(c * rows + q * ln_rows + r * 16, 16), 16)
            dst = pl.ds(pl.multiple_of(q * ln_rows + r * 16, 16), 16)
            tot = jnp.zeros((16, lane), jnp.float32)
            for j in range(n_lane):
                tot = tot + xbuf[src, j * lane:(j + 1) * lane].astype(jnp.float32)
            mean = jnp.sum(tot, axis=-1, keepdims=True) * (1.0 / width)
            var = jnp.zeros((16, lane), jnp.float32)
            for j in range(n_lane):
                cen = xbuf[src, j * lane:(j + 1) * lane].astype(jnp.float32) - mean
                var = var + cen * cen
            rstd = lax.rsqrt(jnp.sum(var, axis=-1, keepdims=True) * (1.0 / width) + LN_EPS)
            for j in range(n_lane):
                for i in range(lane // 128):
                    at = j * lane + i * 128
                    row = slice(at // 128, at // 128 + 1)
                    cl = slice(at, at + 128)
                    cen = xbuf[src, cl].astype(jnp.float32) - mean
                    h = ((cen * rstd) * gains[which, row, :] + biases[which, row, :]).astype(jnp.bfloat16)
                    lhs[0, dst, cl] = h
                    hf = h.astype(jnp.float32)
                    acc8[:, cl] = acc8[:, cl] + (hf[0:8] + hf[8:16])
            return carry

        lax.fori_loop(0, ln_rows // 16, group, 0)

        @pl.when(lax.rem(q, seq_parts) == seq_parts - 1)
        def _():
            m = jnp.sum(acc8[...], axis=0, keepdims=True) * (1.0 / n_seq)
            pay[:, width:2 * width] = pay[:, width:2 * width] + m * m

    def mlp_block(k):
        slot = lax.rem(n_att + k, 2)
        kk = lax.rem(k, 2 * n_blk)
        c = lax.div(k, 2 * n_blk)
        second = lax.div(kk, n_blk)
        b = kk - second * n_blk
        w_copy(wup_hbm, b, slot).wait()
        acc = jnp.dot(lhs[second], wbuf[slot], preferred_element_type=jnp.float32)

        @pl.when(second == 0)
        def _():
            relu = jnp.maximum(acc, 0.0)
            act = relu * relu
            cols = pl.ds(pl.multiple_of(b * bw, bw), bw)
            m0 = jnp.sum(act[0:n_seq], axis=0, keepdims=True) * (1.0 / n_seq)
            m1 = jnp.sum(act[n_seq:rows], axis=0, keepdims=True) * (1.0 / n_seq)
            pay[:, cols] = pay[:, cols] + (m0 * m0 + m1 * m1)
            lhs[1, :, cols] = act.astype(jnp.bfloat16)

        @pl.when(second == 1)
        def _():
            for g in range(2):
                for half in range(2):
                    part[(2 * c + g) * n_items + 2 * b + half] = acc[
                        g * n_seq:(g + 1) * n_seq, half * cw:(half + 1) * cw
                    ]

        start_block(n_att + k + 2)

    def pay_copy(peer, src_d, o):
        return pltpu.make_async_remote_copy(
            src_ref=pay, dst_ref=recvpay.at[src_d], send_sem=p_send.at[o], recv_sem=p_recv.at[src_d],
            device_id={"dp": peer}, device_id_type=MESH,
        )

    first = -(n_pre + 1 + LN_PARTS)
    ln_at = n_items - 1 + lag
    mlp_at = ln_at + LN_PARTS
    pay_at = mlp_at + n_mlp - n_blk + 2

    def step(i, carry):
        s = i + first

        @pl.when(s >= 0)
        def _():
            service(s)

        starts = (first, LN1_AT, ln_at, ln_at + n_items)
        on = [(s >= at) & (s < at + LN_PARTS) for at in starts]

        @pl.when(on[0] | on[1] | on[2] | on[3])
        def _():
            at = jnp.where(on[0], starts[0], jnp.where(on[1], starts[1], jnp.where(on[2], starts[2], starts[3])))
            ln_part(jnp.where(on[2] | on[3], 1, 0), jnp.where(on[1] | on[3], 1, 0), s - at)

        @pl.when(s == 0)
        def _():
            x_copy(1).wait()

        idx = s - first - LN_PARTS

        @pl.when((idx >= 0) & (idx < n_att))
        def _():
            att_block(idx)

        k = s - mlp_at

        @pl.when((k >= 0) & (k < n_mlp))
        def _():
            mlp_block(k)

        @pl.when(s == pay_at)
        def _():
            for o in range(1, dp):
                pay_copy(lax.rem(d + o, dp), d, o).start()
            recvpay[d] = pay[...]

        return carry

    lax.fori_loop(0, total + lag - first, step, 0)

    for o in range(1, dp):
        src_d = lax.rem(d + o, dp)
        pay_copy(src_d, src_d, o).wait_recv()
    score = recvpay[0]
    for j in range(1, dp):
        score = score + recvpay[j]
    score_ref[...] = jnp.sqrt(score)
    for o in range(1, dp):
        pay_copy(lax.rem(d + o, dp), d, o).wait_send()
    for g in range(2):
        p = place(g)
        for back in range(SLOTS):
            t = total - 1 - back
            slot = t % SLOTS

            @pl.when(p == 0)
            def _(g=g, t=t, slot=slot):
                r_copy(g, t, part.at[0]).wait_send()

            if back < SKEW:
                @pl.when((p == 1) | (p == 2))
                def _(g=g, t=t, slot=slot):
                    r_copy(g, t, rslot.at[g, slot]).wait_send()
                    b_copy(g, t, bslot.at[g, slot]).wait_send()

                @pl.when(p == last)
                def _(g=g, t=t, slot=slot):
                    b_copy(g, t, rslot.at[g, slot]).wait_send()


def layer(tp, dp, n_seq, x_rows, w_q, w_k, w_v, w_o, w_up, w_down, norms, rope):
    tokens, width = x_rows.shape
    k_attn = w_q.shape[1]
    kv_width = w_k.shape[1]
    cw = ITEM_COLS
    n_items = width // cw
    dims = (tp, dp, n_seq, width, k_attn, kv_width, n_items)
    rows = 2 * n_seq
    pay = (1, 2 * width + HEAD_DIM)
    hbm = pl.BlockSpec(memory_space=pl.ANY)
    vmem = pl.BlockSpec(memory_space=pltpu.VMEM)
    dma = pltpu.SemaphoreType.DMA
    return pl.pallas_call(
        functools.partial(layer_kernel, dims),
        name="layer",
        out_shape=(
            pltpu.VMEM((tokens, width), jnp.bfloat16),
            pltpu.VMEM(pay, jnp.float32),
        ),
        in_specs=[hbm] * 7 + [vmem] * 6,
        out_specs=(vmem, vmem),
        scratch_shapes=[
            pltpu.VMEM((rows, k_attn), jnp.bfloat16),
            pltpu.VMEM((2, kv_width // HEAD_DIM, n_seq, HEAD_DIM), jnp.bfloat16),
            pltpu.VMEM((2, kv_width // HEAD_DIM, n_seq, HEAD_DIM), jnp.bfloat16),
            pltpu.VMEM((2, width // 128, 128), jnp.float32),
            pltpu.VMEM((2, width // 128, 128), jnp.float32),
            pltpu.VMEM((tokens // n_seq * n_items, n_seq, cw), jnp.float32),
            pltpu.VMEM((2, rows, width), jnp.bfloat16),
            pltpu.VMEM((2, width, 2 * cw), jnp.bfloat16),
            pltpu.VMEM((2, SLOTS, n_seq, cw), jnp.float32),
            pltpu.VMEM((2, SLOTS, n_seq, cw), jnp.float32),
            pltpu.VMEM((8, width), jnp.float32),
            pltpu.VMEM(pay, jnp.float32),
            pltpu.VMEM((dp,) + pay, jnp.float32),
            dma((2,)), dma((3,)),
            dma((2, SLOTS)), dma((2, SLOTS)), dma((2, SLOTS)), dma((2, SLOTS)),
            dma((dp,)), dma((dp,)),
            pltpu.SemaphoreType.REGULAR((2,)), pltpu.SemaphoreType.REGULAR((2,)),
        ],
        compiler_params=pltpu.CompilerParams(
            collective_id=0, has_side_effects=True, vmem_limit_bytes=VMEM_BYTES
        ),
        cost_estimate=pl.CostEstimate(
            flops=4 * tokens * width * (k_attn + kv_width + width),
            bytes_accessed=4 * width * (2 * k_attn + 2 * kv_width + 2 * width),
            transcendentals=0,
        ),
    )(x_rows, w_q, w_k, w_v, w_o, w_up, w_down, *norms, *rope)


def solution(mesh):
    tp = mesh.shape["tp"]
    dp = mesh.shape["dp"]

    def local_layer(hidden, positions, ln1_gain, ln1_bias, w_q, w_k, w_v, w_o, ln2_gain, ln2_bias, w_up, w_down):
        n_batch, n_seq, width = hidden.shape
        ff_local = w_up.shape[1]
        heads = w_q.shape[1] // HEAD_DIM
        y_rows, score = layer(
            tp, dp, n_seq, hidden.reshape(n_batch * n_seq, width), w_q, w_k, w_v, w_o, w_up, w_down,
            [v.reshape(width // 128, 128) for v in (ln1_gain, ln1_bias, ln2_gain, ln2_bias)],
            rope_tables(positions),
        )
        roots = score.reshape(-1)
        return (
            y_rows.reshape(n_batch, n_seq, width),
            roots[:ff_local],
            roots[ff_local + width:ff_local + width + heads],
            roots[ff_local:ff_local + width],
        )

    weight_col = P(None, "tp")
    weight_row = P("tp", None)
    return jax.shard_map(
        local_layer,
        mesh=mesh,
        in_specs=(P("dp"), P(), P(), P(), weight_col, weight_col, weight_col, weight_row, P(), P(), weight_col, weight_row),
        out_specs=(P("dp"), P("tp"), P("tp"), P()),
        check_vma=False,
    )
```

```python
import functools

import jax
import jax.numpy as jnp
from jax import lax
from jax.experimental import pallas as pl
from jax.experimental.pallas import tpu as pltpu
from jax.sharding import PartitionSpec as P

HEAD_DIM = 128
ROT_DIM = 64
ROPE_BASE = 10000.0
LN_EPS = 1e-5
MESH = pl.DeviceIdType.MESH

BLOCK_COLS = 512
ITEM_COLS = 128
TURNS = 2
SKEW = 2
SLOTS = 8
LN_PARTS = 4
VMEM_BYTES = 52 << 20
LN1_AT = 8


def rope_tables(positions):
    rot_half = ROT_DIM // 2
    lane_id = jnp.arange(HEAD_DIM)
    pair = (lane_id % rot_half).astype(jnp.float32)
    inv_freq = ROPE_BASE ** (-2.0 * pair / ROT_DIM)
    pos_angle = positions.astype(jnp.float32)[:, None] * inv_freq[None, :]
    sign = jnp.where(lane_id < rot_half, -1.0, 1.0)
    return jnp.cos(pos_angle), jnp.sin(pos_angle) * sign[None, :]


def layer_kernel(
    dims,
    x_hbm, wq_hbm, wk_hbm, wv_hbm, wo_hbm, wup_hbm, wdn_hbm, gain1_ref, bias1_ref, gain2_ref, bias2_ref, cos_ref, sin_ref,
    xbuf, score_ref,
    attn, kbuf, vbuf, gains, biases, part, lhs, wbuf, rslot, bslot, pay, recvpay,
    in_sem, w_sem, r_send, r_recv, b_send, b_recv, p_send, p_recv, r_cred, b_cred,
):
    tp, dp, n_seq, width, k_attn, kv_width, n_items = dims
    n_chunks = 2
    z = lax.axis_index("tp")
    d = lax.axis_index("dp")
    last = tp - 1
    cw = width // n_items
    bw = BLOCK_COLS
    per = bw // cw
    n_blk = width // bw
    rows = 2 * n_seq
    total = 2 * n_chunks * n_items
    lag = 2 * last * SKEW

    barrier = pltpu.get_barrier_semaphore()
    for o in range(1, tp):
        pl.semaphore_signal(barrier, inc=1, device_id={"tp": lax.rem(z + o, tp)}, device_id_type=MESH)
    for o in range(1, dp):
        pl.semaphore_signal(barrier, inc=1, device_id={"dp": lax.rem(d + o, dp)}, device_id_type=MESH)

    ln_rows = rows // LN_PARTS

    def x_copy(q):
        r = pl.ds(pl.multiple_of(q * ln_rows, ln_rows), ln_rows)
        return pltpu.make_async_copy(x_hbm.at[r, :], xbuf.at[r, :], in_sem.at[q])

    rest = pl.ds(rows, rows)
    x_rest = pltpu.make_async_copy(x_hbm.at[rest, :], xbuf.at[rest, :], in_sem.at[LN_PARTS])

    heads_blk = bw // HEAD_DIM
    n_q = k_attn // bw
    n_pre = 1 + n_q
    att_len = n_pre + n_blk
    n_att = n_chunks * att_len
    q_group = k_attn // kv_width

    def w_copy(hbm, b, slot):
        cols = pl.ds(pl.multiple_of(b * bw, bw), bw)
        return pltpu.make_async_copy(hbm.at[:, cols], wbuf.at[slot], w_sem.at[slot])

    def wo_copy(b, slot):
        cols = pl.ds(pl.multiple_of(b * bw, bw), bw)
        return pltpu.make_async_copy(wo_hbm.at[:, cols], wbuf.at[slot, pl.ds(0, k_attn), :], w_sem.at[slot])

    def k_copy(slot):
        return pltpu.make_async_copy(wk_hbm, wbuf.at[slot, :, pl.ds(0, kv_width)], w_sem.at[slot])

    def v_copy(slot):
        return pltpu.make_async_copy(wv_hbm, wbuf.at[slot, :, pl.ds(kv_width, kv_width)], w_sem.at[2])

    def start_block(idx):
        slot = lax.rem(idx, 2)

        @pl.when(idx < n_att)
        def _():
            j = lax.rem(idx, att_len)

            @pl.when(j == 0)
            def _():
                k_copy(slot).start()
                v_copy(slot).start()

            @pl.when((j > 0) & (j < n_pre))
            def _():
                w_copy(wq_hbm, j - 1, slot).start()

            @pl.when(j >= n_pre)
            def _():
                wo_copy(j - n_pre, slot).start()

        @pl.when((idx >= n_att) & (idx < n_att + n_mlp))
        def _():
            kk = lax.rem(idx - n_att, 2 * n_blk)

            @pl.when(kk < n_blk)
            def _():
                w_copy(wup_hbm, kk, slot).start()

            @pl.when(kk >= n_blk)
            def _():
                w_copy(wdn_hbm, kk - n_blk, slot).start()

    def rotate(heads):
        reps = heads.shape[0] // n_seq
        lane_id = lax.broadcasted_iota(jnp.int32, heads.shape, 1)
        quarter = ROT_DIM // 2
        partner = jnp.where(
            lane_id < quarter, pltpu.roll(heads, HEAD_DIM - quarter, 1), pltpu.roll(heads, quarter, 1)
        )
        cos_t = jnp.concatenate([cos_ref[...]] * reps, axis=0)
        sin_t = jnp.concatenate([sin_ref[...]] * reps, axis=0)
        return jnp.where(lane_id < ROT_DIM, heads * cos_t + partner * sin_t, heads).astype(jnp.bfloat16)

    def keys_values(slot):
        k_copy(slot).wait()
        v_copy(slot).wait()
        acc = jnp.dot(lhs[0], wbuf[slot], preferred_element_type=jnp.float32).astype(jnp.bfloat16)
        for g in range(2):
            r = slice(g * n_seq, (g + 1) * n_seq)
            for h in range(kv_width // HEAD_DIM):
                cl = slice(h * HEAD_DIM, (h + 1) * HEAD_DIM)
                kbuf[g, h] = rotate(acc[r, cl].astype(jnp.float32))
                vbuf[g, h] = acc[r, kv_width + h * HEAD_DIM:kv_width + (h + 1) * HEAD_DIM]

    def queries(jq, slot):
        w_copy(wq_hbm, jq, slot).wait()
        acc = jnp.dot(lhs[0], wbuf[slot], preferred_element_type=jnp.float32).astype(jnp.bfloat16)
        kv = lax.div(jq * heads_blk, q_group)
        shape = (heads_blk * n_seq, n_seq)
        causal = lax.rem(lax.broadcasted_iota(jnp.int32, shape, 0), n_seq) >= lax.broadcasted_iota(jnp.int32, shape, 1)
        for g in range(2):
            r = slice(g * n_seq, (g + 1) * n_seq)
            heads = jnp.concatenate(
                [acc[r, h * HEAD_DIM:(h + 1) * HEAD_DIM].astype(jnp.float32) for h in range(heads_blk)], axis=0
            )
            q_rot = rotate(heads)
            logits = lax.dot_general(
                q_rot, kbuf[g, kv], (((1,), (1,)), ((), ())), preferred_element_type=jnp.float32
            ) * HEAD_DIM ** -0.5
            logits = jnp.where(causal, logits, -1e30)
            weights = jnp.exp(logits - jnp.max(logits, axis=-1, keepdims=True))
            prob = (weights / jnp.sum(weights, axis=-1, keepdims=True)).astype(jnp.bfloat16)
            out = jnp.dot(prob, vbuf[g, kv], preferred_element_type=jnp.float32).astype(jnp.bfloat16)
            for h in range(heads_blk):
                cl = pl.ds(pl.multiple_of(jq * bw + h * HEAD_DIM, HEAD_DIM), HEAD_DIM)
                attn[r, cl] = out[h * n_seq:(h + 1) * n_seq]

    def head_scores():
        lane_id = lax.broadcasted_iota(jnp.int32, (1, HEAD_DIM), 1)

        def some_heads(j, head_sq):
            for h in range(heads_blk):
                head = j * heads_blk + h
                cl = pl.ds(pl.multiple_of(head * HEAD_DIM, HEAD_DIM), HEAD_DIM)
                for g in range(2):
                    wide = attn[g * n_seq:(g + 1) * n_seq, cl].astype(jnp.float32)
                    norm = jnp.sqrt(jnp.sum(wide * wide, axis=-1, keepdims=True))
                    m = jnp.sum(norm, axis=0, keepdims=True) * (1.0 / n_seq)
                    head_sq = head_sq + jnp.where(lane_id == head, m * m, 0.0)
            return head_sq

        at = slice(2 * width, 2 * width + HEAD_DIM)
        pay[:, at] = pay[:, at] + lax.fori_loop(0, n_q, some_heads, jnp.zeros((1, HEAD_DIM), jnp.float32))

    def embed_scores():
        def some_columns(j, carry):
            cl = pl.ds(pl.multiple_of(j * bw, bw), bw)
            m = [
                jnp.sum(lhs[0, g * n_seq:(g + 1) * n_seq, cl].astype(jnp.float32), axis=0, keepdims=True) * (1.0 / n_seq)
                for g in range(2)
            ]
            out = pl.ds(pl.multiple_of(width + j * bw, bw), bw)
            pay[:, out] = pay[:, out] + (m[0] * m[0] + m[1] * m[1])
            return carry

        lax.fori_loop(0, n_blk, some_columns, 0)

    def out_proj(c, b, slot):
        wo_copy(b, slot).wait()
        acc = jnp.dot(attn[...], wbuf[slot, 0:k_attn, :], preferred_element_type=jnp.float32)
        for g in range(2):
            for q in range(per):
                part[(2 * c + g) * n_items + per * b + q] = acc[g * n_seq:(g + 1) * n_seq, q * cw:(q + 1) * cw]

    def att_block(idx):
        slot = lax.rem(idx, 2)
        c = lax.div(idx, att_len)
        j = lax.rem(idx, att_len)

        @pl.when(j == 0)
        def _():
            keys_values(slot)

        @pl.when((j > 0) & (j < n_pre))
        def _():
            queries(j - 1, slot)

        @pl.when(j >= n_pre)
        def _():
            out_proj(c, j - n_pre, slot)

        start_block(idx + 2)

    n_mlp = 2 * n_blk * n_chunks
    for q in range(LN_PARTS):
        x_copy(q).start()
    start_block(jnp.int32(0))
    start_block(jnp.int32(1))
    x_rest.start()
    pay[...] = jnp.zeros_like(pay)
    for which, (gain, bias) in enumerate(((gain1_ref, bias1_ref), (gain2_ref, bias2_ref))):
        gains[which] = 1.0 + gain[...].astype(jnp.float32)
        biases[which] = bias[...].astype(jnp.float32)
    pl.semaphore_wait(barrier, tp - 1 + dp - 1)

    def tile_of(t, g):
        c = lax.rem(lax.div(t, n_items), n_chunks)
        i = lax.rem(t, n_items)
        row = pl.multiple_of((2 * c + g) * n_seq, n_seq)
        col = pl.multiple_of(i * cw, cw)
        return (2 * c + g) * n_items + i, pl.ds(row, n_seq), pl.ds(col, cw)

    def place(g):
        return z if g == 0 else last - z

    def onward(g):
        return {"tp": z + 1} if g == 0 else {"tp": z - 1}

    def backward(g):
        return {"tp": z - 1} if g == 0 else {"tp": z + 1}

    def r_copy(g, t, src):
        slot = lax.rem(t, SLOTS)
        return pltpu.make_async_remote_copy(
            src_ref=src, dst_ref=rslot.at[g, slot], send_sem=r_send.at[g, slot], recv_sem=r_recv.at[g, slot],
            device_id=onward(g), device_id_type=MESH,
        )

    def b_copy(g, t, src):
        slot = lax.rem(t, SLOTS)
        return pltpu.make_async_remote_copy(
            src_ref=src, dst_ref=bslot.at[g, slot], send_sem=b_send.at[g, slot], recv_sem=b_recv.at[g, slot],
            device_id=backward(g), device_id_type=MESH,
        )

    def r_arrive(g, t, p):
        slot = lax.rem(t, SLOTS)
        idx, rws, cls = tile_of(t, g)

        @pl.when((p == 1) | (p == 2))
        def _():
            r_copy(g, t, rslot.at[g, slot]).wait_recv()
            rslot[g, slot] = rslot[g, slot] + part[idx]

        @pl.when(p == last)
        def _():
            r_copy(g, t, rslot.at[g, slot]).wait_recv()
            new = (xbuf[rws, cls].astype(jnp.float32) + (rslot[g, slot] + part[idx])).astype(jnp.bfloat16)
            xbuf[rws, cls] = new
            rslot[g, slot] = new.astype(jnp.float32)

    def r_leave(g, t, p):
        slot = lax.rem(t, SLOTS)
        old = t - SKEW
        old_slot = lax.rem(old + SLOTS, SLOTS)
        idx, _, _ = tile_of(t, g)

        @pl.when((p == 0) & (t >= SLOTS))
        def _():
            r_copy(g, t, part.at[idx]).wait_send()

        @pl.when((p < last) & (t >= SLOTS))
        def _():
            pl.semaphore_wait(r_cred.at[g], 1)

        @pl.when(p == 0)
        def _():
            r_copy(g, t, part.at[idx]).start()

        @pl.when((p == 1) | (p == 2))
        def _():
            r_copy(g, t, rslot.at[g, slot]).start()

        @pl.when((p == last) & (t >= SLOTS))
        def _():
            pl.semaphore_wait(b_cred.at[g], 1)

        @pl.when(p == last)
        def _():
            b_copy(g, t, rslot.at[g, slot]).start()

        @pl.when(((p == 1) | (p == 2)) & (old >= 0))
        def _():
            r_copy(g, old, rslot.at[g, old_slot]).wait_send()

        @pl.when((p == last) & (old >= 0))
        def _():
            b_copy(g, old, rslot.at[g, old_slot]).wait_send()

        @pl.when((p > 0) & (old >= 0) & (old < total - SLOTS))
        def _():
            pl.semaphore_signal(r_cred.at[g], inc=1, device_id=backward(g), device_id_type=MESH)

    def b_step(g, t, p):
        slot = lax.rem(t, SLOTS)
        old = t - SKEW
        old_slot = lax.rem(old + SLOTS, SLOTS)
        _, rws, cls = tile_of(t, g)
        b_copy(g, t, bslot.at[g, slot]).wait_recv()

        @pl.when((p > 0) & (t >= SLOTS))
        def _():
            pl.semaphore_wait(b_cred.at[g], 1)

        @pl.when(p > 0)
        def _():
            b_copy(g, t, bslot.at[g, slot]).start()

        xbuf[rws, cls] = bslot[g, slot].astype(jnp.bfloat16)

        @pl.when((p > 0) & (old >= 0))
        def _():
            b_copy(g, old, bslot.at[g, old_slot]).wait_send()

        @pl.when((old >= 0) & (old < total - SLOTS))
        def _():
            pl.semaphore_signal(b_cred.at[g], inc=1, device_id=onward(g), device_id_type=MESH)

    def service(s):
        for g in range(2):
            p = place(g)
            t = s - SKEW * p

            @pl.when((t >= 0) & (t < total))
            def _(g=g, p=p, t=t):
                r_arrive(g, t, p)

        for g in range(2):
            p = place(g)
            t = s - SKEW * (2 * last - p)

            @pl.when((p < last) & (t >= 0) & (t < total))
            def _(g=g, p=p, t=t):
                b_step(g, t, p)

        for g in range(2):
            p = place(g)
            t = s - SKEW * p

            @pl.when((t >= 0) & (t < total))
            def _(g=g, p=p, t=t):
                r_leave(g, t, p)

    lane = 512 if width % 512 == 0 else 128
    n_lane = width // lane

    def ln_part(which, c, q):
        def group(r, carry):
            src = pl.ds(pl.multiple_of(c * rows + q * ln_rows + r * 16, 16), 16)
            dst = pl.ds(pl.multiple_of(q * ln_rows + r * 16, 16), 16)
            tot = jnp.zeros((16, lane), jnp.float32)
            for j in range(n_lane):
                tot = tot + xbuf[src, j * lane:(j + 1) * lane].astype(jnp.float32)
            mean = jnp.sum(tot, axis=-1, keepdims=True) * (1.0 / width)
            var = jnp.zeros((16, lane), jnp.float32)
            for j in range(n_lane):
                cen = xbuf[src, j * lane:(j + 1) * lane].astype(jnp.float32) - mean
                var = var + cen * cen
            rstd = lax.rsqrt(jnp.sum(var, axis=-1, keepdims=True) * (1.0 / width) + LN_EPS)
            for j in range(n_lane):
                for i in range(lane // 128):
                    at = j * lane + i * 128
                    row = slice(at // 128, at // 128 + 1)
                    cl = slice(at, at + 128)
                    cen = xbuf[src, cl].astype(jnp.float32) - mean
                    h = ((cen * rstd) * gains[which, row, :] + biases[which, row, :]).astype(jnp.bfloat16)
                    lhs[0, dst, cl] = h
            return carry

        lax.fori_loop(0, ln_rows // 16, group, 0)

    def mlp_block(k):
        slot = lax.rem(n_att + k, 2)
        kk = lax.rem(k, 2 * n_blk)
        c = lax.div(k, 2 * n_blk)
        second = lax.div(kk, n_blk)
        b = kk - second * n_blk
        w_copy(wup_hbm, b, slot).wait()
        acc = jnp.dot(lhs[second], wbuf[slot], preferred_element_type=jnp.float32)

        @pl.when(second == 0)
        def _():
            relu = jnp.maximum(acc, 0.0)
            act = relu * relu
            cols = pl.ds(pl.multiple_of(b * bw, bw), bw)
            m0 = jnp.sum(act[0:n_seq], axis=0, keepdims=True) * (1.0 / n_seq)
            m1 = jnp.sum(act[n_seq:rows], axis=0, keepdims=True) * (1.0 / n_seq)
            pay[:, cols] = pay[:, cols] + (m0 * m0 + m1 * m1)
            lhs[1, :, cols] = act.astype(jnp.bfloat16)

        @pl.when(second == 1)
        def _():
            for g in range(2):
                for q in range(per):
                    part[(2 * c + g) * n_items + per * b + q] = acc[g * n_seq:(g + 1) * n_seq, q * cw:(q + 1) * cw]

        start_block(n_att + k + 2)

    def pay_copy(peer, src_d, o):
        return pltpu.make_async_remote_copy(
            src_ref=pay, dst_ref=recvpay.at[src_d], send_sem=p_send.at[o], recv_sem=p_recv.at[src_d],
            device_id={"dp": peer}, device_id_type=MESH,
        )

    first = -(n_pre + 1 + LN_PARTS)
    span = n_items // TURNS
    ln_at = -(-(n_items - TURNS + lag) // TURNS)
    mlp_at = ln_at + LN_PARTS
    pay_at = mlp_at + n_mlp - n_blk + 2

    def turn(i, carry):
        u = i + first * TURNS

        @pl.when(u >= 0)
        def _():
            service(u)

        @pl.when(lax.rem(i, TURNS) == TURNS - 1)
        def _():
            step(lax.div(i, TURNS) + first)

        return carry

    def step(s):
        starts = (first, LN1_AT, ln_at, ln_at + span)
        on = [(s >= at) & (s < at + LN_PARTS) for at in starts]

        @pl.when(on[0])
        def _():
            x_copy(s - first).wait()

        @pl.when(on[0] | on[1] | on[2] | on[3])
        def _():
            at = jnp.where(on[0], starts[0], jnp.where(on[1], starts[1], jnp.where(on[2], starts[2], starts[3])))
            ln_part(jnp.where(on[2] | on[3], 1, 0), jnp.where(on[1] | on[3], 1, 0), s - at)

        @pl.when(s == 0)
        def _():
            x_rest.wait()

        @pl.when((s == LN1_AT - 2) | (s == LN1_AT + LN_PARTS) | (s == mlp_at) | (s == mlp_at + span))
        def _():
            embed_scores()

        @pl.when((s == LN1_AT + LN_PARTS + 1) | (s == n_att - n_pre - 1))
        def _():
            head_scores()

        idx = s - first - LN_PARTS

        @pl.when((idx >= 0) & (idx < n_att))
        def _():
            att_block(idx)

        k = s - mlp_at

        @pl.when((k >= 0) & (k < n_mlp))
        def _():
            mlp_block(k)

        @pl.when(s == pay_at)
        def _():
            for o in range(1, dp):
                pay_copy(lax.rem(d + o, dp), d, o).start()
            recvpay[d] = pay[...]

    lax.fori_loop(0, total + lag - first * TURNS, turn, 0)

    for o in range(1, dp):
        src_d = lax.rem(d + o, dp)
        pay_copy(src_d, src_d, o).wait_recv()
    score = recvpay[0]
    for j in range(1, dp):
        score = score + recvpay[j]
    score_ref[...] = jnp.sqrt(score)
    for o in range(1, dp):
        pay_copy(lax.rem(d + o, dp), d, o).wait_send()
    for g in range(2):
        p = place(g)
        for back in range(SLOTS):
            t = total - 1 - back
            slot = t % SLOTS

            @pl.when(p == 0)
            def _(g=g, t=t, slot=slot):
                r_copy(g, t, part.at[0]).wait_send()

            if back < SKEW:
                @pl.when((p == 1) | (p == 2))
                def _(g=g, t=t, slot=slot):
                    r_copy(g, t, rslot.at[g, slot]).wait_send()
                    b_copy(g, t, bslot.at[g, slot]).wait_send()

                @pl.when(p == last)
                def _(g=g, t=t, slot=slot):
                    b_copy(g, t, rslot.at[g, slot]).wait_send()


def layer(tp, dp, n_seq, x_rows, w_q, w_k, w_v, w_o, w_up, w_down, norms, rope):
    tokens, width = x_rows.shape
    k_attn = w_q.shape[1]
    kv_width = w_k.shape[1]
    cw = ITEM_COLS
    n_items = width // cw
    dims = (tp, dp, n_seq, width, k_attn, kv_width, n_items)
    rows = 2 * n_seq
    pay = (1, 2 * width + HEAD_DIM)
    hbm = pl.BlockSpec(memory_space=pl.ANY)
    vmem = pl.BlockSpec(memory_space=pltpu.VMEM)
    dma = pltpu.SemaphoreType.DMA
    return pl.pallas_call(
        functools.partial(layer_kernel, dims),
        name="layer",
        out_shape=(
            pltpu.VMEM((tokens, width), jnp.bfloat16),
            pltpu.VMEM(pay, jnp.float32),
        ),
        in_specs=[hbm] * 7 + [vmem] * 6,
        out_specs=(vmem, vmem),
        scratch_shapes=[
            pltpu.VMEM((rows, k_attn), jnp.bfloat16),
            pltpu.VMEM((2, kv_width // HEAD_DIM, n_seq, HEAD_DIM), jnp.bfloat16),
            pltpu.VMEM((2, kv_width // HEAD_DIM, n_seq, HEAD_DIM), jnp.bfloat16),
            pltpu.VMEM((2, width // 128, 128), jnp.float32),
            pltpu.VMEM((2, width // 128, 128), jnp.float32),
            pltpu.VMEM((tokens // n_seq * n_items, n_seq, cw), jnp.float32),
            pltpu.VMEM((2, rows, width), jnp.bfloat16),
            pltpu.VMEM((2, width, BLOCK_COLS), jnp.bfloat16),
            pltpu.VMEM((2, SLOTS, n_seq, cw), jnp.float32),
            pltpu.VMEM((2, SLOTS, n_seq, cw), jnp.float32),
            pltpu.VMEM(pay, jnp.float32),
            pltpu.VMEM((dp,) + pay, jnp.float32),
            dma((LN_PARTS + 1,)), dma((3,)),
            dma((2, SLOTS)), dma((2, SLOTS)), dma((2, SLOTS)), dma((2, SLOTS)),
            dma((dp,)), dma((dp,)),
            pltpu.SemaphoreType.REGULAR((2,)), pltpu.SemaphoreType.REGULAR((2,)),
        ],
        compiler_params=pltpu.CompilerParams(
            collective_id=0, has_side_effects=True, vmem_limit_bytes=VMEM_BYTES
        ),
        cost_estimate=pl.CostEstimate(
            flops=4 * tokens * width * (k_attn + kv_width + width),
            bytes_accessed=4 * width * (2 * k_attn + 2 * kv_width + 2 * width),
            transcendentals=0,
        ),
    )(x_rows, w_q, w_k, w_v, w_o, w_up, w_down, *norms, *rope)


def solution(mesh):
    tp = mesh.shape["tp"]
    dp = mesh.shape["dp"]

    def local_layer(hidden, positions, ln1_gain, ln1_bias, w_q, w_k, w_v, w_o, ln2_gain, ln2_bias, w_up, w_down):
        n_batch, n_seq, width = hidden.shape
        ff_local = w_up.shape[1]
        heads = w_q.shape[1] // HEAD_DIM
        y_rows, score = layer(
            tp, dp, n_seq, hidden.reshape(n_batch * n_seq, width), w_q, w_k, w_v, w_o, w_up, w_down,
            [v.reshape(width // 128, 128) for v in (ln1_gain, ln1_bias, ln2_gain, ln2_bias)],
            rope_tables(positions),
        )
        roots = score.reshape(-1)
        return (
            y_rows.reshape(n_batch, n_seq, width),
            roots[:ff_local],
            roots[ff_local + width:ff_local + width + heads],
            roots[ff_local:ff_local + width],
        )

    weight_col = P(None, "tp")
    weight_row = P("tp", None)
    return jax.shard_map(
        local_layer,
        mesh=mesh,
        in_specs=(P("dp"), P(), P(), P(), weight_col, weight_col, weight_col, weight_row, P(), P(), weight_col, weight_row),
        out_specs=(P("dp"), P("tp"), P("tp"), P()),
        check_vma=False,
    )
```

```python
import functools

import jax
import jax.numpy as jnp
from jax import lax
from jax.experimental import pallas as pl
from jax.experimental.pallas import tpu as pltpu
from jax.sharding import PartitionSpec as P

HEAD_DIM = 128
ROT_DIM = 64
ROPE_BASE = 10000.0
LN_EPS = 1e-5
MESH = pl.DeviceIdType.MESH

BLOCK_COLS = 512
ITEM_COLS = 128
TURNS = 2
SKEW = 3
SLOTS = 12
LN_PARTS = 4
VMEM_BYTES = 52 << 20
LN1_AT = 8


def rope_tables(positions):
    rot_half = ROT_DIM // 2
    lane_id = jnp.arange(HEAD_DIM)
    pair = (lane_id % rot_half).astype(jnp.float32)
    inv_freq = ROPE_BASE ** (-2.0 * pair / ROT_DIM)
    pos_angle = positions.astype(jnp.float32)[:, None] * inv_freq[None, :]
    sign = jnp.where(lane_id < rot_half, -1.0, 1.0)
    return jnp.cos(pos_angle), jnp.sin(pos_angle) * sign[None, :]


def layer_kernel(
    dims,
    x_hbm, wq_hbm, wk_hbm, wv_hbm, wo_hbm, wup_hbm, wdn_hbm, gain1_ref, bias1_ref, gain2_ref, bias2_ref, cos_ref, sin_ref,
    xbuf, score_ref,
    attn, kbuf, vbuf, gains, biases, part, lhs, wbuf, rslot, bslot, pay, recvpay,
    in_sem, w_sem, r_send, r_recv, b_send, b_recv, p_send, p_recv, r_cred, b_cred,
):
    tp, dp, n_seq, width, k_attn, kv_width, n_items = dims
    n_chunks = 2
    z = lax.axis_index("tp")
    d = lax.axis_index("dp")
    last = tp - 1
    cw = width // n_items
    bw = BLOCK_COLS
    per = bw // cw
    n_blk = width // bw
    rows = 2 * n_seq
    total = 2 * n_chunks * n_items
    lag = 2 * last * SKEW

    barrier = pltpu.get_barrier_semaphore()
    for o in range(1, tp):
        pl.semaphore_signal(barrier, inc=1, device_id={"tp": lax.rem(z + o, tp)}, device_id_type=MESH)
    for o in range(1, dp):
        pl.semaphore_signal(barrier, inc=1, device_id={"dp": lax.rem(d + o, dp)}, device_id_type=MESH)

    ln_rows = rows // LN_PARTS

    def x_copy(q):
        r = pl.ds(pl.multiple_of(q * ln_rows, ln_rows), ln_rows)
        return pltpu.make_async_copy(x_hbm.at[r, :], xbuf.at[r, :], in_sem.at[q])

    rest = pl.ds(rows, rows)
    x_rest = pltpu.make_async_copy(x_hbm.at[rest, :], xbuf.at[rest, :], in_sem.at[LN_PARTS])

    heads_blk = bw // HEAD_DIM
    n_q = k_attn // bw
    n_pre = 1 + n_q
    att_len = n_pre + n_blk
    n_att = n_chunks * att_len
    q_group = k_attn // kv_width

    def w_copy(hbm, b, slot):
        cols = pl.ds(pl.multiple_of(b * bw, bw), bw)
        return pltpu.make_async_copy(hbm.at[:, cols], wbuf.at[slot], w_sem.at[slot])

    def wo_copy(b, slot):
        cols = pl.ds(pl.multiple_of(b * bw, bw), bw)
        return pltpu.make_async_copy(wo_hbm.at[:, cols], wbuf.at[slot, pl.ds(0, k_attn), :], w_sem.at[slot])

    def k_copy(slot):
        return pltpu.make_async_copy(wk_hbm, wbuf.at[slot, :, pl.ds(0, kv_width)], w_sem.at[slot])

    def v_copy(slot):
        return pltpu.make_async_copy(wv_hbm, wbuf.at[slot, :, pl.ds(kv_width, kv_width)], w_sem.at[2])

    def start_block(idx):
        slot = lax.rem(idx, 2)

        @pl.when(idx < n_att)
        def _():
            j = lax.rem(idx, att_len)

            @pl.when(j == 0)
            def _():
                k_copy(slot).start()
                v_copy(slot).start()

            @pl.when((j > 0) & (j < n_pre))
            def _():
                w_copy(wq_hbm, j - 1, slot).start()

            @pl.when(j >= n_pre)
            def _():
                wo_copy(j - n_pre, slot).start()

        @pl.when((idx >= n_att) & (idx < n_att + n_mlp))
        def _():
            kk = lax.rem(idx - n_att, 2 * n_blk)

            @pl.when(kk < n_blk)
            def _():
                w_copy(wup_hbm, kk, slot).start()

            @pl.when(kk >= n_blk)
            def _():
                w_copy(wdn_hbm, kk - n_blk, slot).start()

    def rotate(heads):
        reps = heads.shape[0] // n_seq
        lane_id = lax.broadcasted_iota(jnp.int32, heads.shape, 1)
        quarter = ROT_DIM // 2
        partner = jnp.where(
            lane_id < quarter, pltpu.roll(heads, HEAD_DIM - quarter, 1), pltpu.roll(heads, quarter, 1)
        )
        cos_t = jnp.concatenate([cos_ref[...]] * reps, axis=0)
        sin_t = jnp.concatenate([sin_ref[...]] * reps, axis=0)
        return jnp.where(lane_id < ROT_DIM, heads * cos_t + partner * sin_t, heads).astype(jnp.bfloat16)

    def keys_values(slot):
        k_copy(slot).wait()
        v_copy(slot).wait()
        acc = jnp.dot(lhs[0], wbuf[slot], preferred_element_type=jnp.float32).astype(jnp.bfloat16)
        for g in range(2):
            r = slice(g * n_seq, (g + 1) * n_seq)
            for h in range(kv_width // HEAD_DIM):
                cl = slice(h * HEAD_DIM, (h + 1) * HEAD_DIM)
                kbuf[g, h] = rotate(acc[r, cl].astype(jnp.float32))
                vbuf[g, h] = acc[r, kv_width + h * HEAD_DIM:kv_width + (h + 1) * HEAD_DIM]

    def queries(jq, slot):
        w_copy(wq_hbm, jq, slot).wait()
        acc = jnp.dot(lhs[0], wbuf[slot], preferred_element_type=jnp.float32).astype(jnp.bfloat16)
        kv = lax.div(jq * heads_blk, q_group)
        shape = (heads_blk * n_seq, n_seq)
        causal = lax.rem(lax.broadcasted_iota(jnp.int32, shape, 0), n_seq) >= lax.broadcasted_iota(jnp.int32, shape, 1)
        for g in range(2):
            r = slice(g * n_seq, (g + 1) * n_seq)
            heads = jnp.concatenate(
                [acc[r, h * HEAD_DIM:(h + 1) * HEAD_DIM].astype(jnp.float32) for h in range(heads_blk)], axis=0
            )
            q_rot = rotate(heads)
            logits = lax.dot_general(
                q_rot, kbuf[g, kv], (((1,), (1,)), ((), ())), preferred_element_type=jnp.float32
            ) * HEAD_DIM ** -0.5
            logits = jnp.where(causal, logits, -1e30)
            weights = jnp.exp(logits - jnp.max(logits, axis=-1, keepdims=True))
            prob = (weights / jnp.sum(weights, axis=-1, keepdims=True)).astype(jnp.bfloat16)
            out = jnp.dot(prob, vbuf[g, kv], preferred_element_type=jnp.float32).astype(jnp.bfloat16)
            for h in range(heads_blk):
                cl = pl.ds(pl.multiple_of(jq * bw + h * HEAD_DIM, HEAD_DIM), HEAD_DIM)
                attn[r, cl] = out[h * n_seq:(h + 1) * n_seq]

    def head_scores():
        lane_id = lax.broadcasted_iota(jnp.int32, (1, HEAD_DIM), 1)

        def some_heads(j, head_sq):
            for h in range(heads_blk):
                head = j * heads_blk + h
                cl = pl.ds(pl.multiple_of(head * HEAD_DIM, HEAD_DIM), HEAD_DIM)
                for g in range(2):
                    wide = attn[g * n_seq:(g + 1) * n_seq, cl].astype(jnp.float32)
                    norm = jnp.sqrt(jnp.sum(wide * wide, axis=-1, keepdims=True))
                    m = jnp.sum(norm, axis=0, keepdims=True) * (1.0 / n_seq)
                    head_sq = head_sq + jnp.where(lane_id == head, m * m, 0.0)
            return head_sq

        at = slice(2 * width, 2 * width + HEAD_DIM)
        pay[:, at] = pay[:, at] + lax.fori_loop(0, n_q, some_heads, jnp.zeros((1, HEAD_DIM), jnp.float32))

    def embed_scores():
        def some_columns(j, carry):
            cl = pl.ds(pl.multiple_of(j * bw, bw), bw)
            m = [
                jnp.sum(lhs[0, g * n_seq:(g + 1) * n_seq, cl].astype(jnp.float32), axis=0, keepdims=True) * (1.0 / n_seq)
                for g in range(2)
            ]
            out = pl.ds(pl.multiple_of(width + j * bw, bw), bw)
            pay[:, out] = pay[:, out] + (m[0] * m[0] + m[1] * m[1])
            return carry

        lax.fori_loop(0, n_blk, some_columns, 0)

    def out_proj(c, b, slot):
        wo_copy(b, slot).wait()
        acc = jnp.dot(attn[...], wbuf[slot, 0:k_attn, :], preferred_element_type=jnp.float32)
        for g in range(2):
            for q in range(per):
                part[(2 * c + g) * n_items + per * b + q] = acc[g * n_seq:(g + 1) * n_seq, q * cw:(q + 1) * cw]

    def att_block(idx):
        slot = lax.rem(idx, 2)
        c = lax.div(idx, att_len)
        j = lax.rem(idx, att_len)

        @pl.when(j == 0)
        def _():
            keys_values(slot)

        @pl.when((j > 0) & (j < n_pre))
        def _():
            queries(j - 1, slot)

        @pl.when(j >= n_pre)
        def _():
            out_proj(c, j - n_pre, slot)

        start_block(idx + 2)

    n_mlp = 2 * n_blk * n_chunks
    for q in range(LN_PARTS):
        x_copy(q).start()
    pay[...] = jnp.zeros_like(pay)
    for which, (gain, bias) in enumerate(((gain1_ref, bias1_ref), (gain2_ref, bias2_ref))):
        gains[which] = 1.0 + gain[...].astype(jnp.float32)
        biases[which] = bias[...].astype(jnp.float32)
    pl.semaphore_wait(barrier, tp - 1 + dp - 1)

    def tile_of(t, g):
        c = lax.rem(lax.div(t, n_items), n_chunks)
        i = lax.rem(t, n_items)
        row = pl.multiple_of((2 * c + g) * n_seq, n_seq)
        col = pl.multiple_of(i * cw, cw)
        return (2 * c + g) * n_items + i, pl.ds(row, n_seq), pl.ds(col, cw)

    def place(g):
        return z if g == 0 else last - z

    def onward(g):
        return {"tp": z + 1} if g == 0 else {"tp": z - 1}

    def backward(g):
        return {"tp": z - 1} if g == 0 else {"tp": z + 1}

    def r_copy(g, t, src):
        slot = lax.rem(t, SLOTS)
        return pltpu.make_async_remote_copy(
            src_ref=src, dst_ref=rslot.at[g, slot], send_sem=r_send.at[g, slot], recv_sem=r_recv.at[g, slot],
            device_id=onward(g), device_id_type=MESH,
        )

    def b_copy(g, t, src):
        slot = lax.rem(t, SLOTS)
        return pltpu.make_async_remote_copy(
            src_ref=src, dst_ref=bslot.at[g, slot], send_sem=b_send.at[g, slot], recv_sem=b_recv.at[g, slot],
            device_id=backward(g), device_id_type=MESH,
        )

    def r_arrive(g, t, p):
        slot = lax.rem(t, SLOTS)
        idx, rws, cls = tile_of(t, g)

        @pl.when((p == 1) | (p == 2))
        def _():
            r_copy(g, t, rslot.at[g, slot]).wait_recv()
            rslot[g, slot] = rslot[g, slot] + part[idx]

        @pl.when(p == last)
        def _():
            r_copy(g, t, rslot.at[g, slot]).wait_recv()
            new = (xbuf[rws, cls].astype(jnp.float32) + (rslot[g, slot] + part[idx])).astype(jnp.bfloat16)
            xbuf[rws, cls] = new
            rslot[g, slot] = new.astype(jnp.float32)

    def r_leave(g, t, p):
        slot = lax.rem(t, SLOTS)
        old = t - SKEW
        old_slot = lax.rem(old + SLOTS, SLOTS)
        idx, _, _ = tile_of(t, g)

        @pl.when((p == 0) & (t >= SLOTS))
        def _():
            r_copy(g, t, part.at[idx]).wait_send()

        @pl.when((p < last) & (t >= SLOTS))
        def _():
            pl.semaphore_wait(r_cred.at[g], 1)

        @pl.when(p == 0)
        def _():
            r_copy(g, t, part.at[idx]).start()

        @pl.when((p == 1) | (p == 2))
        def _():
            r_copy(g, t, rslot.at[g, slot]).start()

        @pl.when((p == last) & (t >= SLOTS))
        def _():
            pl.semaphore_wait(b_cred.at[g], 1)

        @pl.when(p == last)
        def _():
            b_copy(g, t, rslot.at[g, slot]).start()

        @pl.when(((p == 1) | (p == 2)) & (old >= 0))
        def _():
            r_copy(g, old, rslot.at[g, old_slot]).wait_send()

        @pl.when((p == last) & (old >= 0))
        def _():
            b_copy(g, old, rslot.at[g, old_slot]).wait_send()

        @pl.when((p > 0) & (old >= 0) & (old < total - SLOTS))
        def _():
            pl.semaphore_signal(r_cred.at[g], inc=1, device_id=backward(g), device_id_type=MESH)

    def b_step(g, t, p):
        slot = lax.rem(t, SLOTS)
        old = t - SKEW
        old_slot = lax.rem(old + SLOTS, SLOTS)
        _, rws, cls = tile_of(t, g)
        b_copy(g, t, bslot.at[g, slot]).wait_recv()

        @pl.when((p > 0) & (t >= SLOTS))
        def _():
            pl.semaphore_wait(b_cred.at[g], 1)

        @pl.when(p > 0)
        def _():
            b_copy(g, t, bslot.at[g, slot]).start()

        xbuf[rws, cls] = bslot[g, slot].astype(jnp.bfloat16)

        @pl.when((p > 0) & (old >= 0))
        def _():
            b_copy(g, old, bslot.at[g, old_slot]).wait_send()

        @pl.when((old >= 0) & (old < total - SLOTS))
        def _():
            pl.semaphore_signal(b_cred.at[g], inc=1, device_id=onward(g), device_id_type=MESH)

    def service(s):
        for g in range(2):
            p = place(g)
            t = s - SKEW * p

            @pl.when((t >= 0) & (t < total))
            def _(g=g, p=p, t=t):
                r_arrive(g, t, p)

        for g in range(2):
            p = place(g)
            t = s - SKEW * (2 * last - p)

            @pl.when((p < last) & (t >= 0) & (t < total))
            def _(g=g, p=p, t=t):
                b_step(g, t, p)

        for g in range(2):
            p = place(g)
            t = s - SKEW * p

            @pl.when((t >= 0) & (t < total))
            def _(g=g, p=p, t=t):
                r_leave(g, t, p)

    lane = 512 if width % 512 == 0 else 128
    n_lane = width // lane

    def ln_part(which, c, q):
        def group(r, carry):
            src = pl.ds(pl.multiple_of(c * rows + q * ln_rows + r * 16, 16), 16)
            dst = pl.ds(pl.multiple_of(q * ln_rows + r * 16, 16), 16)
            tot = jnp.zeros((16, lane), jnp.float32)
            for j in range(n_lane):
                tot = tot + xbuf[src, j * lane:(j + 1) * lane].astype(jnp.float32)
            mean = jnp.sum(tot, axis=-1, keepdims=True) * (1.0 / width)
            var = jnp.zeros((16, lane), jnp.float32)
            for j in range(n_lane):
                cen = xbuf[src, j * lane:(j + 1) * lane].astype(jnp.float32) - mean
                var = var + cen * cen
            rstd = lax.rsqrt(jnp.sum(var, axis=-1, keepdims=True) * (1.0 / width) + LN_EPS)
            for j in range(n_lane):
                for i in range(lane // 128):
                    at = j * lane + i * 128
                    row = slice(at // 128, at // 128 + 1)
                    cl = slice(at, at + 128)
                    cen = xbuf[src, cl].astype(jnp.float32) - mean
                    h = ((cen * rstd) * gains[which, row, :] + biases[which, row, :]).astype(jnp.bfloat16)
                    lhs[0, dst, cl] = h
            return carry

        lax.fori_loop(0, ln_rows // 16, group, 0)

    def mlp_block(k):
        slot = lax.rem(n_att + k, 2)
        kk = lax.rem(k, 2 * n_blk)
        c = lax.div(k, 2 * n_blk)
        second = lax.div(kk, n_blk)
        b = kk - second * n_blk
        w_copy(wup_hbm, b, slot).wait()
        acc = jnp.dot(lhs[second], wbuf[slot], preferred_element_type=jnp.float32)

        @pl.when(second == 0)
        def _():
            relu = jnp.maximum(acc, 0.0)
            act = relu * relu
            cols = pl.ds(pl.multiple_of(b * bw, bw), bw)
            m0 = jnp.sum(act[0:n_seq], axis=0, keepdims=True) * (1.0 / n_seq)
            m1 = jnp.sum(act[n_seq:rows], axis=0, keepdims=True) * (1.0 / n_seq)
            pay[:, cols] = pay[:, cols] + (m0 * m0 + m1 * m1)
            lhs[1, :, cols] = act.astype(jnp.bfloat16)

        @pl.when(second == 1)
        def _():
            for g in range(2):
                for q in range(per):
                    part[(2 * c + g) * n_items + per * b + q] = acc[g * n_seq:(g + 1) * n_seq, q * cw:(q + 1) * cw]

        start_block(n_att + k + 2)

    def pay_copy(peer, src_d, o):
        return pltpu.make_async_remote_copy(
            src_ref=pay, dst_ref=recvpay.at[src_d], send_sem=p_send.at[o], recv_sem=p_recv.at[src_d],
            device_id={"dp": peer}, device_id_type=MESH,
        )

    first = -(n_pre + 1 + LN_PARTS)
    span = n_items // TURNS
    ln_at = -(-(n_items - TURNS + lag) // TURNS)
    mlp_at = ln_at + LN_PARTS
    pay_at = mlp_at + n_mlp - n_blk + 2

    def turn(i, carry):
        u = i + first * TURNS

        @pl.when(u >= 0)
        def _():
            service(u)

        @pl.when(lax.rem(i, TURNS) == TURNS - 1)
        def _():
            step(lax.div(i, TURNS) + first)

        return carry

    def step(s):
        starts = (first, LN1_AT, ln_at, ln_at + span)
        on = [(s >= at) & (s < at + LN_PARTS) for at in starts]

        @pl.when(on[0])
        def _():
            x_copy(s - first).wait()

            @pl.when(s < first + 2)
            def _():
                start_block(s - first)

            @pl.when(s == first + LN_PARTS - 1)
            def _():
                x_rest.start()

        @pl.when(on[0] | on[1] | on[2] | on[3])
        def _():
            at = jnp.where(on[0], starts[0], jnp.where(on[1], starts[1], jnp.where(on[2], starts[2], starts[3])))
            ln_part(jnp.where(on[2] | on[3], 1, 0), jnp.where(on[1] | on[3], 1, 0), s - at)

        @pl.when(s == 0)
        def _():
            x_rest.wait()

        @pl.when((s == LN1_AT - 2) | (s == LN1_AT + LN_PARTS) | (s == mlp_at) | (s == mlp_at + span))
        def _():
            embed_scores()

        @pl.when((s == LN1_AT + LN_PARTS + 1) | (s == n_att - n_pre - 1))
        def _():
            head_scores()

        idx = s - first - LN_PARTS

        @pl.when((idx >= 0) & (idx < n_att))
        def _():
            att_block(idx)

        k = s - mlp_at

        @pl.when((k >= 0) & (k < n_mlp))
        def _():
            mlp_block(k)

        @pl.when(s == pay_at)
        def _():
            for o in range(1, dp):
                pay_copy(lax.rem(d + o, dp), d, o).start()
            recvpay[d] = pay[...]

        @pl.when(s == pay_at + 8)
        def _():
            for o in range(1, dp):
                src_d = lax.rem(d + o, dp)
                pay_copy(src_d, src_d, o).wait_recv()
            score = recvpay[0]
            for j in range(1, dp):
                score = score + recvpay[j]
            score_ref[...] = jnp.sqrt(score)

    lax.fori_loop(0, total + lag - first * TURNS, turn, 0)

    for o in range(1, dp):
        pay_copy(lax.rem(d + o, dp), d, o).wait_send()
    for g in range(2):
        p = place(g)
        for back in range(SLOTS):
            t = total - 1 - back
            slot = t % SLOTS

            @pl.when(p == 0)
            def _(g=g, t=t, slot=slot):
                r_copy(g, t, part.at[0]).wait_send()

            if back < SKEW:
                @pl.when((p == 1) | (p == 2))
                def _(g=g, t=t, slot=slot):
                    r_copy(g, t, rslot.at[g, slot]).wait_send()
                    b_copy(g, t, bslot.at[g, slot]).wait_send()

                @pl.when(p == last)
                def _(g=g, t=t, slot=slot):
                    b_copy(g, t, rslot.at[g, slot]).wait_send()


def layer(tp, dp, n_seq, x_rows, w_q, w_k, w_v, w_o, w_up, w_down, norms, rope):
    tokens, width = x_rows.shape
    k_attn = w_q.shape[1]
    kv_width = w_k.shape[1]
    cw = ITEM_COLS
    n_items = width // cw
    dims = (tp, dp, n_seq, width, k_attn, kv_width, n_items)
    rows = 2 * n_seq
    pay = (1, 2 * width + HEAD_DIM)
    hbm = pl.BlockSpec(memory_space=pl.ANY)
    vmem = pl.BlockSpec(memory_space=pltpu.VMEM)
    dma = pltpu.SemaphoreType.DMA
    return pl.pallas_call(
        functools.partial(layer_kernel, dims),
        name="layer",
        out_shape=(
            pltpu.VMEM((tokens, width), jnp.bfloat16),
            pltpu.VMEM(pay, jnp.float32),
        ),
        in_specs=[hbm] * 7 + [vmem] * 6,
        out_specs=(vmem, vmem),
        scratch_shapes=[
            pltpu.VMEM((rows, k_attn), jnp.bfloat16),
            pltpu.VMEM((2, kv_width // HEAD_DIM, n_seq, HEAD_DIM), jnp.bfloat16),
            pltpu.VMEM((2, kv_width // HEAD_DIM, n_seq, HEAD_DIM), jnp.bfloat16),
            pltpu.VMEM((2, width // 128, 128), jnp.float32),
            pltpu.VMEM((2, width // 128, 128), jnp.float32),
            pltpu.VMEM((tokens // n_seq * n_items, n_seq, cw), jnp.float32),
            pltpu.VMEM((2, rows, width), jnp.bfloat16),
            pltpu.VMEM((2, width, BLOCK_COLS), jnp.bfloat16),
            pltpu.VMEM((2, SLOTS, n_seq, cw), jnp.float32),
            pltpu.VMEM((2, SLOTS, n_seq, cw), jnp.float32),
            pltpu.VMEM(pay, jnp.float32),
            pltpu.VMEM((dp,) + pay, jnp.float32),
            dma((LN_PARTS + 1,)), dma((3,)),
            dma((2, SLOTS)), dma((2, SLOTS)), dma((2, SLOTS)), dma((2, SLOTS)),
            dma((dp,)), dma((dp,)),
            pltpu.SemaphoreType.REGULAR((2,)), pltpu.SemaphoreType.REGULAR((2,)),
        ],
        compiler_params=pltpu.CompilerParams(
            collective_id=0, has_side_effects=True, vmem_limit_bytes=VMEM_BYTES
        ),
        cost_estimate=pl.CostEstimate(
            flops=4 * tokens * width * (k_attn + kv_width + width),
            bytes_accessed=4 * width * (2 * k_attn + 2 * kv_width + 2 * width),
            transcendentals=0,
        ),
    )(x_rows, w_q, w_k, w_v, w_o, w_up, w_down, *norms, *rope)


def solution(mesh):
    tp = mesh.shape["tp"]
    dp = mesh.shape["dp"]

    def local_layer(hidden, positions, ln1_gain, ln1_bias, w_q, w_k, w_v, w_o, ln2_gain, ln2_bias, w_up, w_down):
        n_batch, n_seq, width = hidden.shape
        ff_local = w_up.shape[1]
        heads = w_q.shape[1] // HEAD_DIM
        y_rows, score = layer(
            tp, dp, n_seq, hidden.reshape(n_batch * n_seq, width), w_q, w_k, w_v, w_o, w_up, w_down,
            [v.reshape(width // 128, 128) for v in (ln1_gain, ln1_bias, ln2_gain, ln2_bias)],
            rope_tables(positions),
        )
        roots = score.reshape(-1)
        return (
            y_rows.reshape(n_batch, n_seq, width),
            roots[:ff_local],
            roots[ff_local + width:ff_local + width + heads],
            roots[ff_local:ff_local + width],
        )

    weight_col = P(None, "tp")
    weight_row = P("tp", None)
    return jax.shard_map(
        local_layer,
        mesh=mesh,
        in_specs=(P("dp"), P(), P(), P(), weight_col, weight_col, weight_col, weight_row, P(), P(), weight_col, weight_row),
        out_specs=(P("dp"), P("tp"), P("tp"), P()),
        check_vma=False,
    )
```
